256 devices in a mesh: slab: 128 (over z, y, x), comp: 2 (over core).
Axes of the slice: x: 4, y: 4, z: 8, core: 2. Of those that a mesh axis runs over, the one named last changes fastest.
Arguments:
- polarization: float32 [6, 128, 128, 128], P('comp', 'slab'), parts along dimension 0, may hold values from -6 to 6
- inverse_polarizability: float32 [128, 128, 128], P('slab'), may hold values from 0.5 to 2
- occupancy: int32 [128, 16, 16], P('slab'), may hold values 0 or 1
- green_fourier: float32 [6, 256, 256, 256], P(None, 'slab'), may hold values from -12 to 12
Outputs:
- first_image: float32 [6, 128, 128, 128], P('comp', 'slab'), parts along dimension 0
- second_image: float32 [6, 128, 128, 128], P('comp', 'slab'), parts along dimension 0
The draws below stay inside these ranges and needn't reach their ends.
There are 2 independent parts, one for each index of `comp`. The reference program is written for one: setup_inputs(seed, part) draws one part's arguments, and reference() takes and returns one part's arrays. A program takes and returns all parts, laid end to end along the dimension named above; an argument that names none is the same for every part. Nothing has to cross between parts.
All inputs are finite; a program needn't handle non-finite values. No bound on the sum of `occupancy` on one device may be relied on, other than what follows from the above.
Results may differ from the reference program's by a relative error of at most 0.0001.
Values sent between devices are 32-bit elements; how exact they have to be, the bound alone decides.
A program may use at most 64 MiB of HBM per device.

```python
import math
import jax
import jax.numpy as jnp

NY = 128
NZ = 128
BLOCK = 8
MATVECS = 2
NX = 128
LX = 256
LY = 256
LZ = 256


def plant(entries, own_key, smallest, largest):
    index_at = [jax.random.randint(jax.random.fold_in(own_key, axis), (), 0, length) for axis, length in enumerate(entries.shape)]
    main_axis = entries.shape.index(max(entries.shape))
    beside = index_at[:main_axis] + [(index_at[main_axis] + 1) % entries.shape[main_axis]] + index_at[main_axis + 1:]
    return entries.at[tuple(index_at)].set(smallest).at[tuple(beside)].set(largest)


def block_scale(own_key, dims, pieces, least, top_value):
    gain, own = 1.0, jax.random.fold_in(own_key, 6)
    for position, shards_of in pieces:
        heights = jnp.exp(jax.random.uniform(jax.random.fold_in(own, position), (shards_of,), jnp.float32, least / len(pieces), top_value / len(pieces)))
        gain = gain * jnp.repeat(heights, dims[position] // shards_of).reshape([-1 if axis == position else 1 for axis in range(len(dims))])
    return gain


def centred(key, extent, width, reach, shards=(), dtype=jnp.bfloat16):
    factor_of = block_scale(key, extent, shards, -0.22, 0.18) if shards else 1.0
    result = jax.random.normal(key, extent, jnp.float32) * width * factor_of
    return jnp.minimum(jnp.maximum(result, -reach), reach).astype(dtype)


def setup_inputs(seed: int = 0, part: int = 0) -> dict:
    arg_keys = jax.random.split(jax.random.key(seed), 5)
    part_splits = jax.random.split(jax.random.fold_in(arg_keys[4], part), 5)
    polarization = centred(part_splits[0], (3, NX, NY, NZ), 1.0, 6.0, ((1, 128),), jnp.float32)
    inverse_polarizability = jnp.clip(jnp.exp(math.log(2.0) - 1.3862944 * jax.random.uniform(arg_keys[1], (NX, NY, NZ), jnp.float32) ** block_scale(arg_keys[1], (NX, NY, NZ), ((0, 128),), -0.2, 0.2)), 0.5, 2.0)
    occupancy = plant((jax.random.randint(arg_keys[2], (NX, NY // BLOCK, NZ // BLOCK), 0, 4) < 3).astype(jnp.int32), jax.random.fold_in(arg_keys[2], 1), 0, 1)
    green_fourier = centred(arg_keys[3], (6, LZ, LX, LY), 2.0, 12.0, ((1, 128),), jnp.float32)
    return dict(polarization=polarization, inverse_polarizability=inverse_polarizability, occupancy=occupancy, green_fourier=green_fourier)


def expand_mask(occupancy):
    flags = occupancy.astype(jnp.float32)
    first, second, third = flags.shape
    spread = jnp.broadcast_to(flags[:, :, None, :, None], (first, second, BLOCK, third, BLOCK))
    return spread.reshape(first, second * BLOCK, third * BLOCK)


def apply_operator(field, mask, inverse_polarizability, green_ordered):
    masked = field * mask[None]
    padded = jnp.pad(masked, ((0, 0), (0, NX), (0, NY), (0, NZ)))
    spectrum = jnp.fft.fftn(padded, axes=(1, 2, 3))
    combos = ((0, 3, 4), (3, 1, 5), (4, 5, 2))
    results = []
    for row in combos:
        product = green_ordered[row[0]] * spectrum[0] + green_ordered[row[1]] * spectrum[1] + green_ordered[row[2]] * spectrum[2]
        back = jnp.fft.ifftn(product).real[:NX, :NY, :NZ]
        results.append(back.astype(jnp.float32))
    convolved = jnp.stack(results)
    return inverse_polarizability[None] * masked - mask[None] * convolved


def reference(polarization, inverse_polarizability, occupancy, green_fourier):
    mask = expand_mask(occupancy)
    green_ordered = jnp.transpose(green_fourier, (0, 2, 3, 1))
    first_image = apply_operator(polarization, mask, inverse_polarizability, green_ordered)
    current = first_image
    for repeat_index in range(MATVECS - 1):
        current = apply_operator(current, mask, inverse_polarizability, green_ordered)
    return first_image, current
```

```python
import functools

import jax
import jax.numpy as jnp
import numpy as np
from jax import lax
from jax.experimental import pallas as pl
from jax.experimental.pallas import tpu as pltpu
from jax.sharding import PartitionSpec as P

F32 = jnp.float32
BF16 = jnp.bfloat16
MESH = pl.DeviceIdType.MESH


def halves(table):
    table = np.asarray(table, np.float32)
    high = table.astype(BF16)
    low = (table - high.astype(np.float32)).astype(BF16)
    return high, low


def tables(n, padded):
    angle = 2.0 * np.pi / padded * (np.outer(np.arange(padded), np.arange(n)) % padded)
    cosine, sine = np.cos(angle), np.sin(angle)
    wide = np.block([[cosine, sine], [-sine, cosine]])
    planes = np.concatenate([part[kzb::2] for kzb in range(2) for part in (cosine, -sine)])
    return (*halves(wide), *halves(wide.T), *halves(planes), *halves(planes.T))


def split(x):
    high = x.astype(BF16)
    low = (x - high.astype(F32)).astype(BF16)
    return high, low


def dot3(a, b):
    dot = functools.partial(jnp.dot, preferred_element_type=F32)
    return dot(a[0], b[0]) + dot(a[0], b[1]) + dot(a[1], b[0])


def kernel(
    n, pol, inv, occ, green_hbm, wh, wl, th, tl, ph, plo, qh, ql, out,
    green, field, inv_t, mask_t, send, recv, spectrum, send_sem, recv_sem, green_sem,
):
    me = lax.axis_index("slab")
    barrier = pltpu.get_barrier_semaphore()

    @pl.loop(1, n)
    def _(step):
        pl.semaphore_signal(
            barrier, inc=1, device_id={"slab": lax.rem(me + step, n)}, device_id_type=MESH
        )

    green_copy = pltpu.make_async_copy(green_hbm, green, green_sem)
    green_copy.start()

    cells = pol.shape[2]
    blocks = occ.shape[1]
    each = cells // blocks
    spread = (
        lax.broadcasted_iota(jnp.int32, (cells, blocks), 0) // each
        == lax.broadcasted_iota(jnp.int32, (cells, blocks), 1)
    ).astype(F32)
    rows = jnp.dot(spread, occ[0].astype(F32), preferred_element_type=F32)
    mask_t[...] = lax.dot_general(
        spread, rows, (((1,), (1,)), ((), ())), preferred_element_type=F32
    )
    inv_t[...] = inv[0].T
    for c in range(3):
        field[c] = pol[c, 0].T

    wide = (wh, wl)
    tall = (th, tl)

    def exchange(slot):
        @pl.loop(1, n)
        def _(step):
            target = lax.rem(me + step, n)
            pltpu.make_async_remote_copy(
                src_ref=send.at[slot, :, pl.ds(target, 1), :],
                dst_ref=recv.at[slot, :, pl.ds(me, 1), :],
                send_sem=send_sem.at[slot],
                recv_sem=recv_sem.at[slot],
                device_id={"slab": target},
                device_id_type=MESH,
            ).start()

        recv[slot, :, pl.ds(me, 1), :] = send[slot, :, pl.ds(me, 1), :]

    def arrive(slot):
        landed = recv.at[slot, :, pl.ds(0, n - 1), :]
        pltpu.make_async_copy(landed, landed, recv_sem.at[slot]).wait()

    @pl.loop(0, 2)
    def _(turn):
        for c in range(3):
            field[c] = field[c] * mask_t[...]

        @pl.loop(0, 2)
        def _(kzb):
            slot = turn * 4 + kzb
            at = pl.ds(pl.multiple_of(kzb * 2 * n, 2 * n), 2 * n)
            plane = (ph[at, :], plo[at, :])
            for c in range(3):
                send[slot, pl.ds(2 * c, 2)] = dot3(plane, split(field[c])).reshape(2, n, cells)

            @pl.when(slot == 0)
            def _():
                pl.semaphore_wait(barrier, n - 1)

            exchange(slot)

        @pl.when(turn == 0)
        def _():
            green_copy.wait()

        @pl.loop(0, 2)
        def _(kzb):
            slot = turn * 4 + kzb
            arrive(slot)

            @pl.loop(0, 3)
            def _(c):
                rows = recv[slot, pl.ds(2 * c, 2)].reshape(2 * n, cells)
                over_x = dot3((wh[...], wl[...]), split(rows))
                both = jnp.concatenate([over_x[: 2 * n], over_x[2 * n :]], axis=1)
                spectrum[c] = dot3(split(both), (th[...], tl[...]))

            @pl.loop(0, 3)
            def _(a):
                g0 = green[jnp.where(a == 0, 0, a + 2), kzb]
                g1 = green[jnp.where(a == 0, 3, jnp.where(a == 1, 1, 5)), kzb]
                g2 = green[jnp.where(a == 2, 2, a + 4), kzb]
                half = 2 * n
                parts = [
                    g0 * spectrum[0, :, k : k + half]
                    + g1 * spectrum[1, :, k : k + half]
                    + g2 * spectrum[2, :, k : k + half]
                    for k in (0, half)
                ]
                over_y = dot3(split(jnp.concatenate(parts, axis=1)), (wh[...], wl[...]))
                both = jnp.concatenate([over_y[:, :cells], over_y[:, cells:]], axis=0)
                send[slot + 2, pl.ds(2 * a, 2)] = dot3((th[...], tl[...]), split(both)).reshape(
                    2, n, cells
                )

            exchange(slot + 2)

        arrive(turn * 4 + 2)
        arrive(turn * 4 + 3)
        scale = 1.0 / (8 * cells * cells * n)
        for a in range(3):
            total = jnp.zeros((cells, cells), F32)
            for kzb in range(2):
                rows = recv[turn * 4 + 2 + kzb, pl.ds(2 * a, 2)].reshape(2 * n, cells)
                at = slice(kzb * 2 * n, (kzb + 1) * 2 * n)
                total = total + dot3((qh[:, at], ql[:, at]), split(rows))
            image = inv_t[...] * field[a] - mask_t[...] * (total * scale)
            field[a] = image
            out[turn, a, 0] = image.T

    @pl.loop(0, 8)
    def _(slot):
        sent = send.at[slot, :, pl.ds(0, n - 1), :]
        pltpu.make_async_copy(sent, sent, send_sem.at[slot]).wait()


def per_device(n, polarization, inverse_polarizability, occupancy, green_fourier):
    cells = polarization.shape[2]
    padded = green_fourier.shape[2]
    operands = (
        polarization, inverse_polarizability, occupancy, green_fourier, *tables(n, padded)
    )
    vmem = pl.BlockSpec(memory_space=pltpu.VMEM)
    specs = [vmem] * len(operands)
    specs[3] = pl.BlockSpec(memory_space=pl.ANY)
    images = pl.pallas_call(
        functools.partial(kernel, n),
        out_shape=jax.ShapeDtypeStruct((2, *polarization.shape), F32),
        in_specs=specs,
        out_specs=vmem,
        scratch_shapes=[
            pltpu.VMEM(green_fourier.shape, F32),
            pltpu.VMEM((3, cells, cells), F32),
            pltpu.VMEM((cells, cells), F32),
            pltpu.VMEM((cells, cells), F32),
            pltpu.VMEM((8, 6, n, cells), F32),
            pltpu.VMEM((8, 6, n, cells), F32),
            pltpu.VMEM((3, padded, 2 * padded), F32),
            pltpu.SemaphoreType.DMA((8,)),
            pltpu.SemaphoreType.DMA((8,)),
            pltpu.SemaphoreType.DMA,
        ],
        compiler_params=pltpu.CompilerParams(
            has_side_effects=True, collective_id=0, vmem_limit_bytes=56 * 2**20
        ),
    )(*operands)
    return images[0], images[1]


def solution(mesh):
    return jax.shard_map(
        functools.partial(per_device, mesh.shape["slab"]),
        mesh=mesh,
        in_specs=(
            P("comp", "slab", None, None),
            P("slab", None, None),
            P("slab", None, None),
            P(None, "slab", None, None),
        ),
        out_specs=(P("comp", "slab", None, None), P("comp", "slab", None, None)),
        check_vma=False,
    )
```

```python
import functools

import jax
import jax.numpy as jnp
import numpy as np
from jax import lax
from jax.experimental import pallas as pl
from jax.experimental.pallas import tpu as pltpu
from jax.sharding import PartitionSpec as P

F32 = jnp.float32
BF16 = jnp.bfloat16
MESH = pl.DeviceIdType.MESH
ROW = 16
RING = 8
REACH = 4


def halves(table):
    table = np.asarray(table, np.float32)
    high = table.astype(BF16)
    low = (table - high.astype(np.float32)).astype(BF16)
    return high, low


def tables(n, padded):
    angle = 2.0 * np.pi / padded * (np.outer(np.arange(padded), np.arange(n)) % padded)
    cosine, sine = np.cos(angle), np.sin(angle)
    wide = np.block([[cosine, sine], [-sine, cosine]])
    planes = np.stack([part[kzb::2] for kzb in range(2) for part in (cosine, -sine)])
    return (*halves(wide), *halves(wide.T), *halves(planes))


def split(x):
    high = x.astype(BF16)
    low = (x - high.astype(F32)).astype(BF16)
    return high, low


def dot3(a, b):
    dot = functools.partial(jnp.dot, preferred_element_type=F32)
    return dot(a[0], b[0]) + dot(a[0], b[1]) + dot(a[1], b[0])


def kernel(
    n, pol, inv, occ, green_hbm, wh, wl, th, tl, ph, plo, out_0, out_1,
    green, field, inv_t, mask_t, spectrum,
    own_p, side_p, own_q, side_q,
    slab_in, part_out, part_in,
    own_s, side_s, recv, back_s, own_b, side_b,
    fwd_send, fwd_recv, back_send, back_recv, slab_send, slab_recv, part_send, part_recv, green_sem,
):
    me = lax.axis_index("slab")
    row, rank = me // ROW, lax.rem(me, ROW)
    cells = pol.shape[2]

    def at(z_row, r):
        return lax.rem(z_row + 2 * RING, RING) * ROW + r

    step_of = (1, -1)
    sides = (at(row - 1, rank), at(row + 1, rank))

    green_copy = pltpu.make_async_copy(green_hbm, green, green_sem)
    green_copy.start()

    last = (REACH - 1) * ROW
    for slot in range(4):
        for side in range(2):
            side_b[slot, side, :, last:, :] = jnp.zeros((6, ROW, cells), F32)

    barrier = pltpu.get_barrier_semaphore()
    reach = (2 * REACH - 1) * ROW

    @pl.loop(0, reach - 1)
    def _(i):
        j = i + jnp.where(i >= last + rank, 1, 0)
        pl.semaphore_signal(
            barrier,
            inc=1,
            device_id={"slab": lax.rem((row - REACH + 1 + RING) * ROW + j, n)},
            device_id_type=MESH,
        )

    blocks = occ.shape[1]
    each = cells // blocks
    spread = (
        lax.broadcasted_iota(jnp.int32, (cells, blocks), 0) // each
        == lax.broadcasted_iota(jnp.int32, (cells, blocks), 1)
    ).astype(F32)
    rows = jnp.dot(spread, occ[0].astype(F32), preferred_element_type=F32)
    mask_t[...] = lax.dot_general(
        spread, rows, (((1,), (1,)), ((), ())), preferred_element_type=F32
    )
    inv_t[...] = inv[0].T
    for c in range(3):
        field[c] = pol[c, 0].T * mask_t[...]

    for half, table in enumerate((ph, plo)):
        pick = pl.ds(pl.multiple_of(row * ROW, ROW), ROW)
        own_p[half] = table[:, pick, :]
        own_q[half] = own_p[half].astype(F32).reshape(4 * ROW, cells).T.astype(BF16)
        for side in range(2):
            for k in range(REACH):
                pick = pl.ds(pl.multiple_of(at(row + step_of[side] * k, 0), ROW), ROW)
                side_p[half, side, :, k * ROW : (k + 1) * ROW, :] = table[:, pick, :]
            side_q[half, side] = (
                side_p[half, side].astype(F32).reshape(4 * REACH * ROW, cells).T.astype(BF16)
            )

    def slab_copy(turn, c, side):
        return pltpu.make_async_remote_copy(
            src_ref=field.at[turn * 3 + c],
            dst_ref=slab_in.at[turn, side, c],
            send_sem=slab_send.at[turn, side, c],
            recv_sem=slab_recv.at[turn, side, c],
            device_id={"slab": sides[1 - side]},
            device_id_type=MESH,
        )

    def part_copy(turn, a, side):
        return pltpu.make_async_remote_copy(
            src_ref=part_out.at[turn, side, a],
            dst_ref=part_in.at[turn, side, a],
            send_sem=part_send.at[turn, side, a],
            recv_sem=part_recv.at[turn, side, a],
            device_id={"slab": sides[side]},
            device_id_type=MESH,
        )

    def place(ref, slot, lead, index, count):
        return ref.at[slot, pl.ds(lead, count), pl.ds(index, 1), :]

    def send_to(src, dst, target, send_sem, recv_sem):
        pltpu.make_async_remote_copy(
            src_ref=src, dst_ref=dst, send_sem=send_sem, recv_sem=recv_sem,
            device_id={"slab": target}, device_id_type=MESH,
        ).start()

    def messages(own, side):
        @pl.loop(1, ROW, unroll=3)
        def _(i):
            r = rank ^ i
            own(r)
            side(0, 0, r)
            side(1, 0, r)

        @pl.loop(0, ROW, unroll=2)
        def _(r):
            for k in range(1, REACH - 1):
                side(0, k, r)
                side(1, k, r)

        @pl.loop(0, ROW // 2, unroll=2)
        def _(i):
            even = 2 * i + lax.rem(rank, 2)
            side(0, REACH - 1, even)
            side(1, REACH - 1, even ^ 1)

    def forward(slot):
        sems = (fwd_send.at[slot], fwd_recv.at[slot])

        def own(r):
            send_to(
                own_s.at[slot, :, pl.ds(r, 1), :], recv.at[slot, :, pl.ds(me, 1), :],
                row * ROW + r, *sems,
            )

        def side(which, k, r):
            send_to(
                side_s.at[slot, which, :, pl.ds(k * ROW + r, 1), :],
                recv.at[slot, :, pl.ds(sides[which], 1), :],
                at(row + step_of[which] * k, r), *sems,
            )

        messages(own, side)
        recv[slot, :, pl.ds(me, 1), :] = own_s[slot, :, pl.ds(rank, 1), :]
        for which in range(2):
            recv[slot, :, pl.ds(sides[which], 1), :] = side_s[slot, which, :, pl.ds(rank, 1), :]

    count = n - 3

    def forward_wait(slot):
        landed = recv.at[slot, :, pl.ds(0, count), :]
        pltpu.make_async_copy(landed, landed, fwd_recv.at[slot]).wait()

    def backward(slot, a):
        sems = (back_send.at[slot, a], back_recv.at[slot, a])
        pair = pl.ds(2 * a, 2)

        def own(r):
            send_to(
                back_s.at[slot, pair, pl.ds(row * ROW + r, 1), :],
                own_b.at[slot, pair, pl.ds(rank, 1), :],
                row * ROW + r, *sems,
            )

        def side(which, k, r):
            collector = row - step_of[which] * k
            send_to(
                back_s.at[slot, pair, pl.ds(at(collector - step_of[which], r), 1), :],
                side_b.at[slot, which, pair, pl.ds(k * ROW + rank, 1), :],
                at(collector, r), *sems,
            )

        messages(own, side)
        own_b[slot, pair, pl.ds(rank, 1), :] = back_s[slot, pair, pl.ds(me, 1), :]
        for which in range(2):
            side_b[slot, which, pair, pl.ds(rank, 1), :] = back_s[
                slot, pair, pl.ds(sides[which], 1), :
            ]

    def backward_wait(slot, a):
        landed = back_s.at[slot, pl.ds(0, 2), pl.ds(0, count), :]
        pltpu.make_async_copy(landed, landed, back_recv.at[slot, a]).wait()

    pl.semaphore_wait(barrier, reach - 1)
    for c in range(3):
        for side in range(2):
            slab_copy(0, c, side).start()

    scale = 1.0 / (8 * cells * cells * n)

    @pl.loop(0, 2)
    def _(turn):
        for c in range(3):
            for side in range(2):
                slab_copy(turn, c, side).wait_recv()

        @pl.loop(0, 2)
        def _(kzb):
            slot = turn * 2 + kzb
            lead = pl.ds(2 * kzb, 2)
            for c in range(3):
                pair = slice(2 * c, 2 * c + 2)
                lhs = [own_p[half, lead].reshape(2 * ROW, cells) for half in range(2)]
                own_s[slot, pair] = dot3(lhs, split(field[turn * 3 + c])).reshape(2, ROW, cells)
                for side in range(2):
                    lhs = [
                        side_p[half, side, lead].reshape(2 * REACH * ROW, cells)
                        for half in range(2)
                    ]
                    side_s[slot, side, pair] = dot3(lhs, split(slab_in[turn, side, c])).reshape(
                        2, REACH * ROW, cells
                    )
            forward(slot)

        @pl.when(turn == 0)
        def _():
            green_copy.wait()

        @pl.loop(0, 2)
        def _(kzb):
            slot = turn * 2 + kzb
            forward_wait(slot)

            @pl.loop(0, 3)
            def _(c):
                rows = recv[slot, pl.ds(2 * c, 2)].reshape(2 * n, cells)
                over_x = dot3((wh[...], wl[...]), split(rows))
                both = jnp.concatenate([over_x[: 2 * n], over_x[2 * n :]], axis=1)
                spectrum[c] = dot3(split(both), (th[...], tl[...]))

            @pl.loop(0, 3)
            def _(a):
                g0 = green[jnp.where(a == 0, 0, a + 2), kzb]
                g1 = green[jnp.where(a == 0, 3, jnp.where(a == 1, 1, 5)), kzb]
                g2 = green[jnp.where(a == 2, 2, a + 4), kzb]
                half = 2 * n
                parts = [
                    g0 * spectrum[0, :, k : k + half]
                    + g1 * spectrum[1, :, k : k + half]
                    + g2 * spectrum[2, :, k : k + half]
                    for k in (0, half)
                ]
                over_y = dot3(split(jnp.concatenate(parts, axis=1)), (wh[...], wl[...]))
                both = jnp.concatenate([over_y[:, :cells], over_y[:, cells:]], axis=0)
                back_s[slot, pl.ds(2 * a, 2)] = dot3((th[...], tl[...]), split(both)).reshape(
                    2, n, cells
                )
                backward(slot, a)

        def collect(a):
            for kzb in range(2):
                backward_wait(turn * 2 + kzb, a)
            for side in range(2):
                rows = jnp.concatenate(
                    [
                        side_b[turn * 2 + kzb, side, 2 * a : 2 * a + 2].reshape(-1, cells)
                        for kzb in range(2)
                    ]
                )
                part_out[turn, side, a] = dot3([side_q[half, side] for half in range(2)], split(rows))
                part_copy(turn, a, side).start()

        def finish(a):
            rows = jnp.concatenate(
                [
                    own_b[turn * 2 + kzb, 2 * a : 2 * a + 2].reshape(-1, cells)
                    for kzb in range(2)
                ]
            )
            total = dot3([own_q[half] for half in range(2)], split(rows))
            for side in range(2):
                part_copy(turn, a, side).wait_recv()
            total = total + part_in[turn, 0, a] + part_in[turn, 1, a]
            image = inv_t[...] * field[turn * 3 + a] - mask_t[...] * (total * scale)

            @pl.when(turn == 0)
            def _():
                field[3 + a] = image * mask_t[...]
                for side in range(2):
                    slab_copy(1, a, side).start()
                out_0[a, 0] = image.T

            @pl.when(turn == 1)
            def _():
                out_1[a, 0] = image.T

        collect(0)
        collect(1)
        finish(0)
        collect(2)
        finish(1)
        finish(2)

    @pl.loop(0, 4)
    def _(slot):
        sent = recv.at[slot, :, pl.ds(0, count), :]
        pltpu.make_async_copy(sent, sent, fwd_send.at[slot]).wait()
        for a in range(3):
            sent = back_s.at[slot, pl.ds(0, 2), pl.ds(0, count), :]
            pltpu.make_async_copy(sent, sent, back_send.at[slot, a]).wait()

    @pl.loop(0, 2)
    def _(turn):
        for c in range(3):
            for side in range(2):
                slab_copy(turn, c, side).wait_send()
                part_copy(turn, c, side).wait_send()


def per_device(n, polarization, inverse_polarizability, occupancy, green_fourier):
    cells = polarization.shape[2]
    padded = green_fourier.shape[2]
    operands = (
        polarization, inverse_polarizability, occupancy, green_fourier, *tables(n, padded)
    )
    vmem = pl.BlockSpec(memory_space=pltpu.VMEM)
    specs = [vmem] * len(operands)
    specs[3] = pl.BlockSpec(memory_space=pl.ANY)
    span = REACH * ROW
    image = jax.ShapeDtypeStruct(polarization.shape, F32)
    dma = pltpu.SemaphoreType.DMA
    return pl.pallas_call(
        functools.partial(kernel, n),
        out_shape=(image, image),
        in_specs=specs,
        out_specs=(vmem, vmem),
        scratch_shapes=[
            pltpu.VMEM(green_fourier.shape, F32),
            pltpu.VMEM((6, cells, cells), F32),
            pltpu.VMEM((cells, cells), F32),
            pltpu.VMEM((cells, cells), F32),
            pltpu.VMEM((3, padded, 2 * padded), F32),
            pltpu.VMEM((2, 4, ROW, cells), BF16),
            pltpu.VMEM((2, 2, 4, span, cells), BF16),
            pltpu.VMEM((2, cells, 4 * ROW), BF16),
            pltpu.VMEM((2, 2, cells, 4 * span), BF16),
            pltpu.VMEM((2, 2, 3, cells, cells), F32),
            pltpu.VMEM((2, 2, 3, cells, cells), F32),
            pltpu.VMEM((2, 2, 3, cells, cells), F32),
            pltpu.VMEM((4, 6, ROW, cells), F32),
            pltpu.VMEM((4, 2, 6, span, cells), F32),
            pltpu.VMEM((4, 6, n, cells), F32),
            pltpu.VMEM((4, 6, n, cells), F32),
            pltpu.VMEM((4, 6, ROW, cells), F32),
            pltpu.VMEM((4, 2, 6, span, cells), F32),
            dma((4,)), dma((4,)), dma((4, 3)), dma((4, 3)),
            dma((2, 2, 3)), dma((2, 2, 3)), dma((2, 2, 3)), dma((2, 2, 3)), dma,
        ],
        compiler_params=pltpu.CompilerParams(
            has_side_effects=True, collective_id=0, vmem_limit_bytes=56 * 2**20
        ),
    )(*operands)


def solution(mesh):
    return jax.shard_map(
        functools.partial(per_device, mesh.shape["slab"]),
        mesh=mesh,
        in_specs=(
            P("comp", "slab", None, None),
            P("slab", None, None),
            P("slab", None, None),
            P(None, "slab", None, None),
        ),
        out_specs=(P("comp", "slab", None, None), P("comp", "slab", None, None)),
        check_vma=False,
    )
```

```python
import functools

import jax
import jax.numpy as jnp
import numpy as np
from jax import lax
from jax.experimental import pallas as pl
from jax.experimental.pallas import tpu as pltpu
from jax.sharding import PartitionSpec as P

F32 = jnp.float32
BF16 = jnp.bfloat16
MESH = pl.DeviceIdType.MESH
ROW = 16
RING = 8
REACH = 4


def halves(table):
    table = np.asarray(table, np.float32)
    high = table.astype(BF16)
    low = (table - high.astype(np.float32)).astype(BF16)
    return high, low


def tables(n, padded):
    angle = 2.0 * np.pi / padded * (np.outer(np.arange(padded), np.arange(n)) % padded)
    cosine, sine = np.cos(angle), np.sin(angle)
    wide = np.block([[cosine, sine], [-sine, cosine]])
    planes = np.stack([part[kzb::2] for kzb in range(2) for part in (cosine, -sine)])
    return (*halves(wide), *halves(wide.T), *halves(planes))


def split(x):
    high = x.astype(BF16)
    low = (x - high.astype(F32)).astype(BF16)
    return high, low


def dot3(a, b):
    dot = functools.partial(jnp.dot, preferred_element_type=F32)
    return dot(a[0], b[0]) + dot(a[0], b[1]) + dot(a[1], b[0])


def kernel(
    n, pol_hbm, inv_hbm, occ_hbm, green_hbm, wh_hbm, wl_hbm, th_hbm, tl_hbm, ph_hbm, pl_hbm,
    out_0, out_1,
    pol, inv, occ, green, wh, wl, th, tl, ph, plo, over_x, images,
    field, inv_t, mask_t, spectrum,
    own_p, side_p, own_q, side_q,
    slab_in, part_out, part_in,
    own_s, side_s, recv, back_s, own_b, side_b,
    fwd_send, fwd_recv, back_send, back_recv, slab_send, slab_recv, part_send, part_recv, first_sem, later_sem, out_sem,
):
    me = lax.axis_index("slab")
    row, rank = me // ROW, lax.rem(me, ROW)
    cells = pol.shape[2]

    def at(z_row, r):
        return lax.rem(z_row + 2 * RING, RING) * ROW + r

    step_of = (1, -1)
    sides = (at(row - 1, rank), at(row + 1, rank))

    last = (REACH - 1) * ROW
    for slot in range(4):
        for side in range(2):
            side_b[slot, side, :, last:, :] = jnp.zeros((6, ROW, cells), F32)

    barrier = pltpu.get_barrier_semaphore()
    reach = (2 * REACH - 1) * ROW

    @pl.loop(0, reach - 1)
    def _(i):
        j = i + jnp.where(i >= last + rank, 1, 0)
        pl.semaphore_signal(
            barrier,
            inc=1,
            device_id={"slab": lax.rem((row - REACH + 1 + RING) * ROW + j, n)},
            device_id_type=MESH,
        )

    first = [
        pltpu.make_async_copy(src, dst, first_sem.at[i])
        for i, (src, dst) in enumerate(
            ((occ_hbm, occ), (pol_hbm, pol), (ph_hbm, ph), (pl_hbm, plo), (inv_hbm, inv))
        )
    ]
    later = [
        pltpu.make_async_copy(src, dst, later_sem.at[i])
        for i, (src, dst) in enumerate(
            ((wh_hbm, wh), (wl_hbm, wl), (th_hbm, th), (tl_hbm, tl), (green_hbm, green))
        )
    ]
    for copy in (*first, *later):
        copy.start()
    for copy in first:
        copy.wait()

    blocks = occ.shape[1]
    each = cells // blocks
    spread = (
        lax.broadcasted_iota(jnp.int32, (cells, blocks), 0) // each
        == lax.broadcasted_iota(jnp.int32, (cells, blocks), 1)
    ).astype(F32)
    rows = jnp.dot(spread, occ[0].astype(F32), preferred_element_type=F32)
    mask_t[...] = lax.dot_general(
        spread, rows, (((1,), (1,)), ((), ())), preferred_element_type=F32
    )
    inv_t[...] = inv[0].T
    for c in range(3):
        field[c] = pol[c, 0].T * mask_t[...]

    for half, table in enumerate((ph, plo)):
        pick = pl.ds(pl.multiple_of(row * ROW, ROW), ROW)
        own_p[half] = table[:, pick, :]
        own_q[half] = own_p[half].astype(F32).reshape(4 * ROW, cells).T.astype(BF16)
        for side in range(2):
            for k in range(REACH):
                pick = pl.ds(pl.multiple_of(at(row + step_of[side] * k, 0), ROW), ROW)
                side_p[half, side, :, k * ROW : (k + 1) * ROW, :] = table[:, pick, :]
            side_q[half, side] = (
                side_p[half, side].astype(F32).reshape(4 * REACH * ROW, cells).T.astype(BF16)
            )

    def slab_copy(turn, c, side):
        return pltpu.make_async_remote_copy(
            src_ref=field.at[turn * 3 + c],
            dst_ref=slab_in.at[turn, side, c],
            send_sem=slab_send.at[turn, side, c],
            recv_sem=slab_recv.at[turn, side, c],
            device_id={"slab": sides[1 - side]},
            device_id_type=MESH,
        )

    def part_copy(turn, a, side):
        return pltpu.make_async_remote_copy(
            src_ref=part_out.at[turn, side, a],
            dst_ref=part_in.at[turn, side, a],
            send_sem=part_send.at[turn, side, a],
            recv_sem=part_recv.at[turn, side, a],
            device_id={"slab": sides[side]},
            device_id_type=MESH,
        )

    def out_copy(turn, a):
        out = (out_0, out_1)[turn]
        return pltpu.make_async_copy(images.at[turn, a], out.at[a, 0], out_sem.at[turn, a])

    def send_to(src, dst, target, send_sem, recv_sem):
        pltpu.make_async_remote_copy(
            src_ref=src, dst_ref=dst, send_sem=send_sem, recv_sem=recv_sem,
            device_id={"slab": target}, device_id_type=MESH,
        ).start()

    def messages(own, side):
        @pl.loop(1, ROW, unroll=3)
        def _(i):
            r = rank ^ i
            own(r)
            side(0, 0, r)
            side(1, 0, r)

        @pl.loop(0, ROW, unroll=2)
        def _(r):
            for k in range(1, REACH - 1):
                side(0, k, r)
                side(1, k, r)

        @pl.loop(0, ROW // 2, unroll=2)
        def _(i):
            even = 2 * i + lax.rem(rank, 2)
            side(0, REACH - 1, even)
            side(1, REACH - 1, even ^ 1)

    def forward(slot):
        sems = (fwd_send.at[slot], fwd_recv.at[slot])

        def own(r):
            send_to(
                own_s.at[slot, :, pl.ds(r, 1), :], recv.at[slot, :, pl.ds(me, 1), :],
                row * ROW + r, *sems,
            )

        def side(which, k, r):
            send_to(
                side_s.at[slot, which, :, pl.ds(k * ROW + r, 1), :],
                recv.at[slot, :, pl.ds(sides[which], 1), :],
                at(row + step_of[which] * k, r), *sems,
            )

        messages(own, side)
        recv[slot, :, pl.ds(me, 1), :] = own_s[slot, :, pl.ds(rank, 1), :]
        for which in range(2):
            recv[slot, :, pl.ds(sides[which], 1), :] = side_s[slot, which, :, pl.ds(rank, 1), :]

    count = n - 3

    def forward_wait(slot):
        landed = recv.at[slot, :, pl.ds(0, count), :]
        pltpu.make_async_copy(landed, landed, fwd_recv.at[slot]).wait()

    def backward(slot):
        sems = (back_send.at[slot], back_recv.at[slot])

        def own(r):
            send_to(
                back_s.at[slot, :, pl.ds(row * ROW + r, 1), :],
                own_b.at[slot, :, pl.ds(rank, 1), :],
                row * ROW + r, *sems,
            )

        def side(which, k, r):
            collector = row - step_of[which] * k
            send_to(
                back_s.at[slot, :, pl.ds(at(collector - step_of[which], r), 1), :],
                side_b.at[slot, which, :, pl.ds(k * ROW + rank, 1), :],
                at(collector, r), *sems,
            )

        messages(own, side)
        own_b[slot, :, pl.ds(rank, 1), :] = back_s[slot, :, pl.ds(me, 1), :]
        for which in range(2):
            side_b[slot, which, :, pl.ds(rank, 1), :] = back_s[slot, :, pl.ds(sides[which], 1), :]

    def backward_wait(slot):
        landed = back_s.at[slot, :, pl.ds(0, count), :]
        pltpu.make_async_copy(landed, landed, back_recv.at[slot]).wait()

    pl.semaphore_wait(barrier, reach - 1)
    for c in range(3):
        for side in range(2):
            slab_copy(0, c, side).start()

    scale = 1.0 / (8 * cells * cells * n)

    for turn in range(2):
        for c in range(3):
            for side in range(2):
                slab_copy(turn, c, side).wait_recv()

        @pl.loop(0, 2)
        def _(kzb):
            slot = turn * 2 + kzb
            lead = pl.ds(2 * kzb, 2)
            for c in range(3):
                pair = slice(2 * c, 2 * c + 2)
                lhs = [own_p[half, lead].reshape(2 * ROW, cells) for half in range(2)]
                own_s[slot, pair] = dot3(lhs, split(field[turn * 3 + c])).reshape(2, ROW, cells)
                for side in range(2):
                    lhs = [
                        side_p[half, side, lead].reshape(2 * REACH * ROW, cells)
                        for half in range(2)
                    ]
                    side_s[slot, side, pair] = dot3(lhs, split(slab_in[turn, side, c])).reshape(
                        2, REACH * ROW, cells
                    )
            forward(slot)

        if turn == 0:
            for copy in later:
                copy.wait()

        @pl.loop(0, 2)
        def _(kzb):
            slot = turn * 2 + kzb
            forward_wait(slot)
            half = 2 * n
            rows = split(
                jnp.concatenate(
                    [recv[slot, 2 * c : 2 * c + 2].reshape(half, cells) for c in range(3)], axis=1
                )
            )
            for part in range(2):
                at_rows = slice(part * half, (part + 1) * half)
                product = dot3((wh[at_rows], wl[at_rows]), rows)
                for c in range(3):
                    over_x[c, :, part * cells : (part + 1) * cells] = product[
                        :, c * cells : (c + 1) * cells
                    ]
            for c in range(3):
                spectrum[c] = dot3(split(over_x[c]), (th[...], tl[...]))
            for a, combo in enumerate(((0, 3, 4), (3, 1, 5), (4, 5, 2))):
                parts = [
                    green[combo[0], kzb] * spectrum[0, :, k : k + half]
                    + green[combo[1], kzb] * spectrum[1, :, k : k + half]
                    + green[combo[2], kzb] * spectrum[2, :, k : k + half]
                    for k in (0, half)
                ]
                over_y = dot3(split(jnp.concatenate(parts, axis=1)), (wh[...], wl[...]))
                both = jnp.concatenate([over_y[:, :cells], over_y[:, cells:]], axis=0)
                back_s[slot, 2 * a : 2 * a + 2] = dot3((th[...], tl[...]), split(both)).reshape(
                    2, n, cells
                )
            backward(slot)

        slots = (turn * 2, turn * 2 + 1)
        for slot in slots:
            backward_wait(slot)
        for a in range(3):
            for side in range(2):
                rows = jnp.concatenate(
                    [side_b[slot, side, 2 * a : 2 * a + 2].reshape(-1, cells) for slot in slots]
                )
                part_out[turn, side, a] = dot3((side_q[0, side], side_q[1, side]), split(rows))
                part_copy(turn, a, side).start()
        totals = []
        for a in range(3):
            rows = jnp.concatenate(
                [own_b[slot, 2 * a : 2 * a + 2].reshape(-1, cells) for slot in slots]
            )
            totals.append(dot3((own_q[0], own_q[1]), split(rows)))
        for a in range(3):
            for side in range(2):
                part_copy(turn, a, side).wait_recv()
            total = totals[a] + part_in[turn, 0, a] + part_in[turn, 1, a]
            image = inv_t[...] * field[turn * 3 + a] - mask_t[...] * (total * scale)
            if turn == 0:
                field[3 + a] = image * mask_t[...]
                for side in range(2):
                    slab_copy(1, a, side).start()
            images[turn, a] = image.T
            out_copy(turn, a).start()

    @pl.loop(0, 4)
    def _(slot):
        sent = recv.at[slot, :, pl.ds(0, count), :]
        pltpu.make_async_copy(sent, sent, fwd_send.at[slot]).wait()
        pltpu.make_async_copy(sent, sent, back_send.at[slot]).wait()

    for turn in range(2):
        for c in range(3):
            out_copy(turn, c).wait()
            for side in range(2):
                slab_copy(turn, c, side).wait_send()
                part_copy(turn, c, side).wait_send()


def per_device(n, polarization, inverse_polarizability, occupancy, green_fourier):
    cells = polarization.shape[2]
    padded = green_fourier.shape[2]
    operands = (
        polarization, inverse_polarizability, occupancy, green_fourier, *tables(n, padded)
    )
    span = REACH * ROW
    image = jax.ShapeDtypeStruct(polarization.shape, F32)
    dma = pltpu.SemaphoreType.DMA
    anywhere = pl.BlockSpec(memory_space=pl.ANY)
    return pl.pallas_call(
        functools.partial(kernel, n),
        out_shape=(image, image),
        in_specs=[anywhere] * len(operands),
        out_specs=(anywhere, anywhere),
        scratch_shapes=[
            *(pltpu.VMEM(x.shape, x.dtype) for x in operands),
            pltpu.VMEM((3, padded, padded), F32),
            pltpu.VMEM((2, 3, cells, cells), F32),
            pltpu.VMEM((6, cells, cells), F32),
            pltpu.VMEM((cells, cells), F32),
            pltpu.VMEM((cells, cells), F32),
            pltpu.VMEM((3, padded, 2 * padded), F32),
            pltpu.VMEM((2, 4, ROW, cells), BF16),
            pltpu.VMEM((2, 2, 4, span, cells), BF16),
            pltpu.VMEM((2, cells, 4 * ROW), BF16),
            pltpu.VMEM((2, 2, cells, 4 * span), BF16),
            pltpu.VMEM((2, 2, 3, cells, cells), F32),
            pltpu.VMEM((2, 2, 3, cells, cells), F32),
            pltpu.VMEM((2, 2, 3, cells, cells), F32),
            pltpu.VMEM((4, 6, ROW, cells), F32),
            pltpu.VMEM((4, 2, 6, span, cells), F32),
            pltpu.VMEM((4, 6, n, cells), F32),
            pltpu.VMEM((4, 6, n, cells), F32),
            pltpu.VMEM((4, 6, ROW, cells), F32),
            pltpu.VMEM((4, 2, 6, span, cells), F32),
            dma((4,)), dma((4,)), dma((4,)), dma((4,)),
            dma((2, 2, 3)), dma((2, 2, 3)), dma((2, 2, 3)), dma((2, 2, 3)), dma((5,)), dma((5,)), dma((2, 3)),
        ],
        compiler_params=pltpu.CompilerParams(
            has_side_effects=True, collective_id=0, vmem_limit_bytes=56 * 2**20
        ),
    )(*operands)


def solution(mesh):
    return jax.shard_map(
        functools.partial(per_device, mesh.shape["slab"]),
        mesh=mesh,
        in_specs=(
            P("comp", "slab", None, None),
            P("slab", None, None),
            P("slab", None, None),
            P(None, "slab", None, None),
        ),
        out_specs=(P("comp", "slab", None, None), P("comp", "slab", None, None)),
        check_vma=False,
    )
```

```python
import functools

import jax
import jax.numpy as jnp
import numpy as np
from jax import lax
from jax.experimental import pallas as pl
from jax.experimental.pallas import tpu as pltpu
from jax.sharding import PartitionSpec as P

F32 = jnp.float32
BF16 = jnp.bfloat16
MESH = pl.DeviceIdType.MESH
ROW = 16
RING = 8
REACH = 4


def halves(table):
    table = np.asarray(table, np.float32)
    high = table.astype(BF16)
    low = (table - high.astype(np.float32)).astype(BF16)
    return high, low


def tables(n, padded):
    angle = 2.0 * np.pi / padded * (np.outer(np.arange(padded), np.arange(n)) % padded)
    cosine, sine = np.cos(angle), np.sin(angle)
    wide = np.block([[cosine, sine], [-sine, cosine]])
    planes = np.stack([part[kzb::2] for kzb in range(2) for part in (cosine, -sine)])
    return (*halves(wide), *halves(wide.T), *halves(planes))


def split(x):
    high = x.astype(BF16)
    low = (x - high.astype(F32)).astype(BF16)
    return high, low


def dot3(a, b):
    dot = functools.partial(jnp.dot, preferred_element_type=F32)
    return dot(a[0], b[0]) + dot(a[0], b[1]) + dot(a[1], b[0])


def kernel(
    n, pol_hbm, inv_hbm, occ_hbm, green_hbm, wh_hbm, wl_hbm, th_hbm, tl_hbm, ph_hbm, pl_hbm,
    out_0, out_1,
    pol, inv, occ, green, wh, wl, th, tl, ph, plo, over_x, images,
    field, inv_t, mask_t, spectrum,
    own_p, side_p, own_q, side_q,
    slab_in, part_out, part_in,
    own_s, side_s, recv, back_s, own_b, side_b,
    fwd_send, fwd_recv, back_send, back_recv, slab_send, slab_recv, part_send, part_recv, first_sem, later_sem, out_sem,
):
    me = lax.axis_index("slab")
    row, rank = me // ROW, lax.rem(me, ROW)
    cells = pol.shape[2]

    def at(z_row, r):
        return lax.rem(z_row + 2 * RING, RING) * ROW + r

    step_of = (1, -1)
    sides = (at(row - 1, rank), at(row + 1, rank))

    last = (REACH - 1) * ROW
    for slot in range(4):
        for side in range(2):
            side_b[slot, side, :, last:, :] = jnp.zeros((6, ROW, cells), F32)

    barrier = pltpu.get_barrier_semaphore()
    reach = (2 * REACH - 1) * ROW

    @pl.loop(0, reach - 1)
    def _(i):
        j = i + jnp.where(i >= last + rank, 1, 0)
        pl.semaphore_signal(
            barrier,
            inc=1,
            device_id={"slab": lax.rem((row - REACH + 1 + RING) * ROW + j, n)},
            device_id_type=MESH,
        )

    first = [
        pltpu.make_async_copy(src, dst, first_sem.at[i])
        for i, (src, dst) in enumerate(
            ((occ_hbm, occ), (pol_hbm, pol), (ph_hbm, ph), (pl_hbm, plo), (inv_hbm, inv))
        )
    ]
    later = [
        pltpu.make_async_copy(src, dst, later_sem.at[i])
        for i, (src, dst) in enumerate(
            ((wh_hbm, wh), (wl_hbm, wl), (th_hbm, th), (tl_hbm, tl), (green_hbm, green))
        )
    ]
    for copy in (*first, *later):
        copy.start()
    for copy in first:
        copy.wait()

    blocks = occ.shape[1]
    each = cells // blocks
    spread = (
        lax.broadcasted_iota(jnp.int32, (cells, blocks), 0) // each
        == lax.broadcasted_iota(jnp.int32, (cells, blocks), 1)
    ).astype(F32)
    rows = jnp.dot(spread, occ[0].astype(F32), preferred_element_type=F32)
    mask_t[...] = lax.dot_general(
        spread, rows, (((1,), (1,)), ((), ())), preferred_element_type=F32
    )
    inv_t[...] = inv[0].T
    for c in range(3):
        field[c] = pol[c, 0].T * mask_t[...]

    for half, table in enumerate((ph, plo)):
        pick = pl.ds(pl.multiple_of(row * ROW, ROW), ROW)
        own_p[half] = table[:, pick, :]
        own_q[half] = own_p[half].astype(F32).reshape(4 * ROW, cells).T.astype(BF16)
        for side in range(2):
            for k in range(REACH):
                pick = pl.ds(pl.multiple_of(at(row + step_of[side] * k, 0), ROW), ROW)
                side_p[half, side, :, k * ROW : (k + 1) * ROW, :] = table[:, pick, :]
            side_q[half, side] = (
                side_p[half, side].astype(F32).reshape(4 * REACH * ROW, cells).T.astype(BF16)
            )

    def slab_copy(turn, c, side):
        return pltpu.make_async_remote_copy(
            src_ref=field.at[turn * 3 + c],
            dst_ref=slab_in.at[turn, side, c],
            send_sem=slab_send.at[turn, side, c],
            recv_sem=slab_recv.at[turn, side, c],
            device_id={"slab": sides[1 - side]},
            device_id_type=MESH,
        )

    def part_copy(turn, a, side):
        return pltpu.make_async_remote_copy(
            src_ref=part_out.at[turn, side, a],
            dst_ref=part_in.at[turn, side, a],
            send_sem=part_send.at[turn, side, a],
            recv_sem=part_recv.at[turn, side, a],
            device_id={"slab": sides[side]},
            device_id_type=MESH,
        )

    def out_copy(turn, a):
        out = (out_0, out_1)[turn]
        return pltpu.make_async_copy(images.at[turn, a], out.at[a, 0], out_sem.at[turn, a])

    def send_to(src, dst, target, send_sem, recv_sem):
        pltpu.make_async_remote_copy(
            src_ref=src, dst_ref=dst, send_sem=send_sem, recv_sem=recv_sem,
            device_id={"slab": target}, device_id_type=MESH,
        ).start()

    def messages(own, side):
        @pl.loop(1, ROW, unroll=3)
        def _(i):
            r = rank ^ i
            own(r)
            side(0, 0, r)
            side(1, 0, r)

        @pl.loop(0, ROW, unroll=2)
        def _(r):
            for k in range(1, REACH - 1):
                side(0, k, r)
                side(1, k, r)

        @pl.loop(0, ROW // 2, unroll=2)
        def _(i):
            even = 2 * i + lax.rem(rank, 2)
            side(0, REACH - 1, even)
            side(1, REACH - 1, even ^ 1)

    def forward(slot, low, width, sem):
        sems = (fwd_send.at[sem], fwd_recv.at[sem])
        span = pl.ds(low, width)

        def own(r):
            send_to(
                own_s.at[slot, span, pl.ds(r, 1), :], recv.at[slot, span, pl.ds(me, 1), :],
                row * ROW + r, *sems,
            )

        def side(which, k, r):
            send_to(
                side_s.at[slot, which, span, pl.ds(k * ROW + r, 1), :],
                recv.at[slot, span, pl.ds(sides[which], 1), :],
                at(row + step_of[which] * k, r), *sems,
            )

        messages(own, side)
        recv[slot, span, pl.ds(me, 1), :] = own_s[slot, span, pl.ds(rank, 1), :]
        for which in range(2):
            recv[slot, span, pl.ds(sides[which], 1), :] = side_s[
                slot, which, span, pl.ds(rank, 1), :
            ]

    def backward(slot, low, width, sem):
        sems = (back_send.at[sem], back_recv.at[sem])
        span = pl.ds(low, width)

        def own(r):
            send_to(
                back_s.at[slot, span, pl.ds(row * ROW + r, 1), :],
                own_b.at[slot, span, pl.ds(rank, 1), :],
                row * ROW + r, *sems,
            )

        def side(which, k, r):
            collector = row - step_of[which] * k
            send_to(
                back_s.at[slot, span, pl.ds(at(collector - step_of[which], r), 1), :],
                side_b.at[slot, which, span, pl.ds(k * ROW + rank, 1), :],
                at(collector, r), *sems,
            )

        messages(own, side)
        own_b[slot, span, pl.ds(rank, 1), :] = back_s[slot, span, pl.ds(me, 1), :]
        for which in range(2):
            side_b[slot, which, span, pl.ds(rank, 1), :] = back_s[
                slot, span, pl.ds(sides[which], 1), :
            ]

    def wait_for(ref, width, sem):
        bytes_of = ref.at[0, pl.ds(0, width), pl.ds(0, n - 3), :]
        pltpu.make_async_copy(bytes_of, bytes_of, sem).wait()

    fwd_plan = ((0, 0, 2), (0, 2, 2), (0, 4, 2), (1, 0, 6))
    back_plan = ((0, 0, 6), (1, 0, 2), (1, 2, 2), (1, 4, 2))

    pl.semaphore_wait(barrier, reach - 1)
    for c in range(3):
        for side in range(2):
            slab_copy(0, c, side).start()

    scale = 1.0 / (8 * cells * cells * n)

    half = 2 * n
    for turn in range(2):
        slots = (2 * turn, 2 * turn + 1)
        for c in range(3):
            for side in range(2):
                slab_copy(turn, c, side).wait_recv()
            pair = slice(2 * c, 2 * c + 2)
            lhs = [own_p[part].reshape(4 * ROW, cells) for part in range(2)]
            product = dot3(lhs, split(field[turn * 3 + c])).reshape(4, ROW, cells)
            for kzb, slot in enumerate(slots):
                own_s[slot, pair] = product[2 * kzb : 2 * kzb + 2]
            for side in range(2):
                lhs = [side_p[part, side].reshape(4 * REACH * ROW, cells) for part in range(2)]
                product = dot3(lhs, split(slab_in[turn, side, c])).reshape(4, REACH * ROW, cells)
                for kzb, slot in enumerate(slots):
                    side_s[slot, side, pair] = product[2 * kzb : 2 * kzb + 2]
            forward(slots[0], 2 * c, 2, 4 * turn + c)
        forward(slots[1], 0, 6, 4 * turn + 3)

        if turn == 0:
            for copy in later:
                copy.wait()

        for kzb, slot in enumerate(slots):
            for sem, (plane, low, width) in enumerate(fwd_plan):
                if plane == kzb:
                    wait_for(recv, width, fwd_recv.at[4 * turn + sem])
            rows = split(
                jnp.concatenate(
                    [recv[slot, 2 * c : 2 * c + 2].reshape(half, cells) for c in range(3)], axis=1
                )
            )
            for part in range(2):
                at_rows = slice(part * half, (part + 1) * half)
                product = dot3((wh[at_rows], wl[at_rows]), rows)
                for c in range(3):
                    over_x[c, :, part * cells : (part + 1) * cells] = product[
                        :, c * cells : (c + 1) * cells
                    ]
            for c in range(3):
                spectrum[c] = dot3(split(over_x[c]), (th[...], tl[...]))
            for a, combo in enumerate(((0, 3, 4), (3, 1, 5), (4, 5, 2))):
                parts = [
                    green[combo[0], kzb] * spectrum[0, :, k : k + half]
                    + green[combo[1], kzb] * spectrum[1, :, k : k + half]
                    + green[combo[2], kzb] * spectrum[2, :, k : k + half]
                    for k in (0, half)
                ]
                over_y = dot3(split(jnp.concatenate(parts, axis=1)), (wh[...], wl[...]))
                both = jnp.concatenate([over_y[:, :cells], over_y[:, cells:]], axis=0)
                back_s[slot, 2 * a : 2 * a + 2] = dot3((th[...], tl[...]), split(both)).reshape(
                    2, n, cells
                )
                if kzb == 1:
                    backward(slot, 2 * a, 2, 4 * turn + 1 + a)
            if kzb == 0:
                backward(slot, 0, 6, 4 * turn)

        wait_for(recv, 6, back_recv.at[4 * turn])
        totals = []
        for a in range(3):
            wait_for(recv, 2, back_recv.at[4 * turn + 1 + a])
            for side in range(2):
                rows = jnp.concatenate(
                    [side_b[slot, side, 2 * a : 2 * a + 2].reshape(-1, cells) for slot in slots]
                )
                part_out[turn, side, a] = dot3((side_q[0, side], side_q[1, side]), split(rows))
                part_copy(turn, a, side).start()
            rows = jnp.concatenate(
                [own_b[slot, 2 * a : 2 * a + 2].reshape(-1, cells) for slot in slots]
            )
            totals.append(dot3((own_q[0], own_q[1]), split(rows)))
        for a in range(3):
            for side in range(2):
                part_copy(turn, a, side).wait_recv()
            total = totals[a] + part_in[turn, 0, a] + part_in[turn, 1, a]
            image = inv_t[...] * field[turn * 3 + a] - mask_t[...] * (total * scale)
            if turn == 0:
                field[3 + a] = image * mask_t[...]
                for side in range(2):
                    slab_copy(1, a, side).start()
            images[turn, a] = image.T
            out_copy(turn, a).start()

    for turn in range(2):
        for plan, sems in ((fwd_plan, fwd_send), (back_plan, back_send)):
            for sem, (_, _, width) in enumerate(plan):
                wait_for(recv, width, sems.at[4 * turn + sem])

    for turn in range(2):
        for c in range(3):
            out_copy(turn, c).wait()
            for side in range(2):
                slab_copy(turn, c, side).wait_send()
                part_copy(turn, c, side).wait_send()


def per_device(n, polarization, inverse_polarizability, occupancy, green_fourier):
    cells = polarization.shape[2]
    padded = green_fourier.shape[2]
    operands = (
        polarization, inverse_polarizability, occupancy, green_fourier, *tables(n, padded)
    )
    span = REACH * ROW
    image = jax.ShapeDtypeStruct(polarization.shape, F32)
    dma = pltpu.SemaphoreType.DMA
    anywhere = pl.BlockSpec(memory_space=pl.ANY)
    return pl.pallas_call(
        functools.partial(kernel, n),
        out_shape=(image, image),
        in_specs=[anywhere] * len(operands),
        out_specs=(anywhere, anywhere),
        scratch_shapes=[
            *(pltpu.VMEM(x.shape, x.dtype) for x in operands),
            pltpu.VMEM((3, padded, padded), F32),
            pltpu.VMEM((2, 3, cells, cells), F32),
            pltpu.VMEM((6, cells, cells), F32),
            pltpu.VMEM((cells, cells), F32),
            pltpu.VMEM((cells, cells), F32),
            pltpu.VMEM((3, padded, 2 * padded), F32),
            pltpu.VMEM((2, 4, ROW, cells), BF16),
            pltpu.VMEM((2, 2, 4, span, cells), BF16),
            pltpu.VMEM((2, cells, 4 * ROW), BF16),
            pltpu.VMEM((2, 2, cells, 4 * span), BF16),
            pltpu.VMEM((2, 2, 3, cells, cells), F32),
            pltpu.VMEM((2, 2, 3, cells, cells), F32),
            pltpu.VMEM((2, 2, 3, cells, cells), F32),
            pltpu.VMEM((4, 6, ROW, cells), F32),
            pltpu.VMEM((4, 2, 6, span, cells), F32),
            pltpu.VMEM((4, 6, n, cells), F32),
            pltpu.VMEM((4, 6, n, cells), F32),
            pltpu.VMEM((4, 6, ROW, cells), F32),
            pltpu.VMEM((4, 2, 6, span, cells), F32),
            dma((8,)), dma((8,)), dma((8,)), dma((8,)),
            dma((2, 2, 3)), dma((2, 2, 3)), dma((2, 2, 3)), dma((2, 2, 3)), dma((5,)), dma((5,)), dma((2, 3)),
        ],
        compiler_params=pltpu.CompilerParams(
            has_side_effects=True, collective_id=0, vmem_limit_bytes=56 * 2**20
        ),
    )(*operands)


def solution(mesh):
    return jax.shard_map(
        functools.partial(per_device, mesh.shape["slab"]),
        mesh=mesh,
        in_specs=(
            P("comp", "slab", None, None),
            P("slab", None, None),
            P("slab", None, None),
            P(None, "slab", None, None),
        ),
        out_specs=(P("comp", "slab", None, None), P("comp", "slab", None, None)),
        check_vma=False,
    )
```

```python
import functools

import jax
import jax.numpy as jnp
import numpy as np
from jax import lax
from jax.experimental import pallas as pl
from jax.experimental.pallas import tpu as pltpu
from jax.sharding import PartitionSpec as P

F32 = jnp.float32
BF16 = jnp.bfloat16
MESH = pl.DeviceIdType.MESH
ROW = 16
RING = 8
REACH = 4


def halves(table):
    table = np.asarray(table, np.float32)
    high = table.astype(BF16)
    low = (table - high.astype(np.float32)).astype(BF16)
    return high, low


def tables(n, padded):
    angle = 2.0 * np.pi / padded * (np.outer(np.arange(padded), np.arange(n)) % padded)
    cosine, sine = np.cos(angle), np.sin(angle)
    wide = np.block([[cosine, sine], [-sine, cosine]])
    planes = np.stack([part[kzb::2] for kzb in range(2) for part in (cosine, -sine)])
    return (*halves(wide), *halves(wide.T), *halves(planes))


def split(x):
    high = x.astype(BF16)
    low = (x - high.astype(F32)).astype(BF16)
    return high, low


def dot3(a, b):
    dot = functools.partial(jnp.dot, preferred_element_type=F32)
    return dot(a[0], b[0]) + dot(a[0], b[1]) + dot(a[1], b[0])


def kernel(
    n, pol_hbm, inv_hbm, occ_hbm, green_hbm, wh_hbm, wl_hbm, th_hbm, tl_hbm, ph_hbm, pl_hbm,
    out_0, out_1,
    pol, inv, occ, green, wh, wl, th, tl, ph, plo, over_x, images,
    field, inv_t, mask_t, spectrum,
    own_p, side_p, own_q, side_q,
    slab_in, part_out, part_in,
    own_s, side_s, recv, back_s, own_b, side_b,
    fwd_send, fwd_recv, back_send, back_recv, slab_send, slab_recv, part_send, part_recv, first_sem, later_sem, out_sem,
):
    me = lax.axis_index("slab")
    row, rank = me // ROW, lax.rem(me, ROW)
    cells = pol.shape[2]

    def at(z_row, r):
        return lax.rem(z_row + 2 * RING, RING) * ROW + r

    step_of = (1, -1)
    sides = (at(row - 1, rank), at(row + 1, rank))

    last = (REACH - 1) * ROW
    for slot in range(4):
        for side in range(2):
            side_b[slot, side, :, last:, :] = jnp.zeros((6, ROW, cells), F32)

    barrier = pltpu.get_barrier_semaphore()

    def greet(target):
        pl.semaphore_signal(barrier, inc=1, device_id={"slab": target}, device_id_type=MESH)

    for k in range(REACH - 1, 0, -1):

        @pl.loop(0, ROW, unroll=4)
        def _(r):
            greet(at(row + k, r))
            greet(at(row - k, r))

    @pl.loop(1, ROW, unroll=3)
    def _(i):
        greet(row * ROW + (rank ^ i))

    first = [
        pltpu.make_async_copy(src, dst, first_sem.at[i])
        for i, (src, dst) in enumerate(
            ((occ_hbm, occ), (pol_hbm, pol), (ph_hbm, ph), (pl_hbm, plo), (inv_hbm, inv))
        )
    ]
    later = [
        pltpu.make_async_copy(src, dst, later_sem.at[i])
        for i, (src, dst) in enumerate(
            ((wh_hbm, wh), (wl_hbm, wl), (th_hbm, th), (tl_hbm, tl), (green_hbm, green))
        )
    ]
    for copy in (*first, *later):
        copy.start()
    for copy in first:
        copy.wait()

    blocks = occ.shape[1]
    each = cells // blocks
    spread = (
        lax.broadcasted_iota(jnp.int32, (cells, blocks), 0) // each
        == lax.broadcasted_iota(jnp.int32, (cells, blocks), 1)
    ).astype(F32)
    rows = jnp.dot(spread, occ[0].astype(F32), preferred_element_type=F32)
    mask_t[...] = lax.dot_general(
        spread, rows, (((1,), (1,)), ((), ())), preferred_element_type=F32
    )
    inv_t[...] = inv[0].T
    for c in range(3):
        field[c] = pol[c, 0].T * mask_t[...]

    for half, table in enumerate((ph, plo)):
        pick = pl.ds(pl.multiple_of(row * ROW, ROW), ROW)
        own_p[half] = table[:, pick, :]
        own_q[half] = own_p[half].astype(F32).reshape(4 * ROW, cells).T.astype(BF16)
        for side in range(2):
            for k in range(REACH):
                pick = pl.ds(pl.multiple_of(at(row + step_of[side] * k, 0), ROW), ROW)
                side_p[half, side, :, k * ROW : (k + 1) * ROW, :] = table[:, pick, :]
            side_q[half, side] = (
                side_p[half, side].astype(F32).reshape(4 * REACH * ROW, cells).T.astype(BF16)
            )

    def slab_copy(turn, c, side):
        return pltpu.make_async_remote_copy(
            src_ref=field.at[turn * 3 + c],
            dst_ref=slab_in.at[turn, side, c],
            send_sem=slab_send.at[turn, side, c],
            recv_sem=slab_recv.at[turn, side, c],
            device_id={"slab": sides[1 - side]},
            device_id_type=MESH,
        )

    def part_copy(turn, a, side):
        return pltpu.make_async_remote_copy(
            src_ref=part_out.at[turn, side, a],
            dst_ref=part_in.at[turn, side, a],
            send_sem=part_send.at[turn, side, a],
            recv_sem=part_recv.at[turn, side, a],
            device_id={"slab": sides[side]},
            device_id_type=MESH,
        )

    def out_copy(turn, a):
        out = (out_0, out_1)[turn]
        return pltpu.make_async_copy(images.at[turn, a], out.at[a, 0], out_sem.at[turn, a])

    def send_to(src, dst, target, send_sem, recv_sem):
        pltpu.make_async_remote_copy(
            src_ref=src, dst_ref=dst, send_sem=send_sem, recv_sem=recv_sem,
            device_id={"slab": target}, device_id_type=MESH,
        ).start()

    def messages(own, side):
        @pl.loop(0, ROW // 2, unroll=2)
        def _(i):
            even = 2 * i + lax.rem(rank, 2)
            side(0, REACH - 1, even)
            side(1, REACH - 1, even ^ 1)

        for k in range(REACH - 2, 0, -1):

            @pl.loop(0, ROW, unroll=4)
            def _(r):
                side(0, k, r)
                side(1, k, r)

        @pl.loop(1, ROW, unroll=3)
        def _(i):
            r = rank ^ i
            side(0, 0, r)
            side(1, 0, r)
            own(r)

    def forward(slot, low, width, sem):
        sems = (fwd_send.at[sem], fwd_recv.at[sem])
        span = pl.ds(low, width)

        def own(r):
            send_to(
                own_s.at[slot, span, pl.ds(r, 1), :], recv.at[slot, span, pl.ds(me, 1), :],
                row * ROW + r, *sems,
            )

        def side(which, k, r):
            send_to(
                side_s.at[slot, which, span, pl.ds(k * ROW + r, 1), :],
                recv.at[slot, span, pl.ds(sides[which], 1), :],
                at(row + step_of[which] * k, r), *sems,
            )

        messages(own, side)
        recv[slot, span, pl.ds(me, 1), :] = own_s[slot, span, pl.ds(rank, 1), :]
        for which in range(2):
            recv[slot, span, pl.ds(sides[which], 1), :] = side_s[
                slot, which, span, pl.ds(rank, 1), :
            ]

    def backward(slot, low, width, sem):
        sems = (back_send.at[sem], back_recv.at[sem])
        span = pl.ds(low, width)

        def own(r):
            send_to(
                back_s.at[slot, span, pl.ds(row * ROW + r, 1), :],
                own_b.at[slot, span, pl.ds(rank, 1), :],
                row * ROW + r, *sems,
            )

        def side(which, k, r):
            collector = row - step_of[which] * k
            send_to(
                back_s.at[slot, span, pl.ds(at(collector - step_of[which], r), 1), :],
                side_b.at[slot, which, span, pl.ds(k * ROW + rank, 1), :],
                at(collector, r), *sems,
            )

        messages(own, side)
        own_b[slot, span, pl.ds(rank, 1), :] = back_s[slot, span, pl.ds(me, 1), :]
        for which in range(2):
            side_b[slot, which, span, pl.ds(rank, 1), :] = back_s[
                slot, span, pl.ds(sides[which], 1), :
            ]

    def wait_for(ref, width, sem):
        bytes_of = ref.at[0, pl.ds(0, width), pl.ds(0, n - 3), :]
        pltpu.make_async_copy(bytes_of, bytes_of, sem).wait()

    fwd_plan = ((0, 0, 2), (0, 2, 2), (0, 4, 2), (1, 0, 6))
    back_plan = ((0, 0, 6), (1, 0, 2), (1, 2, 2), (1, 4, 2))

    pl.semaphore_wait(barrier, (2 * REACH - 1) * ROW - 1)
    for c in range(3):
        for side in range(2):
            slab_copy(0, c, side).start()

    scale = 1.0 / (8 * cells * cells * n)

    half = 2 * n
    for turn in range(2):
        slots = (2 * turn, 2 * turn + 1)
        for c in range(3):
            for side in range(2):
                slab_copy(turn, c, side).wait_recv()
            pair = slice(2 * c, 2 * c + 2)
            lhs = [own_p[part].reshape(4 * ROW, cells) for part in range(2)]
            product = dot3(lhs, split(field[turn * 3 + c])).reshape(4, ROW, cells)
            for kzb, slot in enumerate(slots):
                own_s[slot, pair] = product[2 * kzb : 2 * kzb + 2]
            for side in range(2):
                lhs = [side_p[part, side].reshape(4 * REACH * ROW, cells) for part in range(2)]
                product = dot3(lhs, split(slab_in[turn, side, c])).reshape(4, REACH * ROW, cells)
                for kzb, slot in enumerate(slots):
                    side_s[slot, side, pair] = product[2 * kzb : 2 * kzb + 2]
            forward(slots[0], 2 * c, 2, 4 * turn + c)
        forward(slots[1], 0, 6, 4 * turn + 3)

        if turn == 0:
            for copy in later:
                copy.wait()

        for kzb, slot in enumerate(slots):
            for sem, (plane, low, width) in enumerate(fwd_plan):
                if plane == kzb:
                    wait_for(recv, width, fwd_recv.at[4 * turn + sem])
            rows = split(
                jnp.concatenate(
                    [recv[slot, 2 * c : 2 * c + 2].reshape(half, cells) for c in range(3)], axis=1
                )
            )
            for part in range(2):
                at_rows = slice(part * half, (part + 1) * half)
                product = dot3((wh[at_rows], wl[at_rows]), rows)
                for c in range(3):
                    over_x[c, :, part * cells : (part + 1) * cells] = product[
                        :, c * cells : (c + 1) * cells
                    ]
            for c in range(3):
                spectrum[c] = dot3(split(over_x[c]), (th[...], tl[...]))
            for a, combo in enumerate(((0, 3, 4), (3, 1, 5), (4, 5, 2))):
                parts = [
                    green[combo[0], kzb] * spectrum[0, :, k : k + half]
                    + green[combo[1], kzb] * spectrum[1, :, k : k + half]
                    + green[combo[2], kzb] * spectrum[2, :, k : k + half]
                    for k in (0, half)
                ]
                over_y = dot3(split(jnp.concatenate(parts, axis=1)), (wh[...], wl[...]))
                both = jnp.concatenate([over_y[:, :cells], over_y[:, cells:]], axis=0)
                back_s[slot, 2 * a : 2 * a + 2] = dot3((th[...], tl[...]), split(both)).reshape(
                    2, n, cells
                )
                if kzb == 1:
                    backward(slot, 2 * a, 2, 4 * turn + 1 + a)
            if kzb == 0:
                backward(slot, 0, 6, 4 * turn)

        wait_for(recv, 6, back_recv.at[4 * turn])
        totals = []
        for a in range(3):
            wait_for(recv, 2, back_recv.at[4 * turn + 1 + a])
            for side in range(2):
                rows = jnp.concatenate(
                    [side_b[slot, side, 2 * a : 2 * a + 2].reshape(-1, cells) for slot in slots]
                )
                part_out[turn, side, a] = dot3((side_q[0, side], side_q[1, side]), split(rows))
                part_copy(turn, a, side).start()
            rows = jnp.concatenate(
                [own_b[slot, 2 * a : 2 * a + 2].reshape(-1, cells) for slot in slots]
            )
            totals.append(dot3((own_q[0], own_q[1]), split(rows)))
        for a in range(3):
            for side in range(2):
                part_copy(turn, a, side).wait_recv()
            total = totals[a] + part_in[turn, 0, a] + part_in[turn, 1, a]
            image = inv_t[...] * field[turn * 3 + a] - mask_t[...] * (total * scale)
            if turn == 0:
                field[3 + a] = image * mask_t[...]
                for side in range(2):
                    slab_copy(1, a, side).start()
            images[turn, a] = image.T
            out_copy(turn, a).start()

    for turn in range(2):
        for plan, sems in ((fwd_plan, fwd_send), (back_plan, back_send)):
            for sem, (_, _, width) in enumerate(plan):
                wait_for(recv, width, sems.at[4 * turn + sem])

    for turn in range(2):
        for c in range(3):
            out_copy(turn, c).wait()
            for side in range(2):
                slab_copy(turn, c, side).wait_send()
                part_copy(turn, c, side).wait_send()


def per_device(n, polarization, inverse_polarizability, occupancy, green_fourier):
    cells = polarization.shape[2]
    padded = green_fourier.shape[2]
    operands = (
        polarization, inverse_polarizability, occupancy, green_fourier, *tables(n, padded)
    )
    span = REACH * ROW
    image = jax.ShapeDtypeStruct(polarization.shape, F32)
    dma = pltpu.SemaphoreType.DMA
    anywhere = pl.BlockSpec(memory_space=pl.ANY)
    return pl.pallas_call(
        functools.partial(kernel, n),
        out_shape=(image, image),
        in_specs=[anywhere] * len(operands),
        out_specs=(anywhere, anywhere),
        scratch_shapes=[
            *(pltpu.VMEM(x.shape, x.dtype) for x in operands),
            pltpu.VMEM((3, padded, padded), F32),
            pltpu.VMEM((2, 3, cells, cells), F32),
            pltpu.VMEM((6, cells, cells), F32),
            pltpu.VMEM((cells, cells), F32),
            pltpu.VMEM((cells, cells), F32),
            pltpu.VMEM((3, padded, 2 * padded), F32),
            pltpu.VMEM((2, 4, ROW, cells), BF16),
            pltpu.VMEM((2, 2, 4, span, cells), BF16),
            pltpu.VMEM((2, cells, 4 * ROW), BF16),
            pltpu.VMEM((2, 2, cells, 4 * span), BF16),
            pltpu.VMEM((2, 2, 3, cells, cells), F32),
            pltpu.VMEM((2, 2, 3, cells, cells), F32),
            pltpu.VMEM((2, 2, 3, cells, cells), F32),
            pltpu.VMEM((4, 6, ROW, cells), F32),
            pltpu.VMEM((4, 2, 6, span, cells), F32),
            pltpu.VMEM((4, 6, n, cells), F32),
            pltpu.VMEM((4, 6, n, cells), F32),
            pltpu.VMEM((4, 6, ROW, cells), F32),
            pltpu.VMEM((4, 2, 6, span, cells), F32),
            dma((8,)), dma((8,)), dma((8,)), dma((8,)),
            dma((2, 2, 3)), dma((2, 2, 3)), dma((2, 2, 3)), dma((2, 2, 3)), dma((5,)), dma((5,)), dma((2, 3)),
        ],
        compiler_params=pltpu.CompilerParams(
            has_side_effects=True, collective_id=0, vmem_limit_bytes=56 * 2**20
        ),
    )(*operands)


def solution(mesh):
    return jax.shard_map(
        functools.partial(per_device, mesh.shape["slab"]),
        mesh=mesh,
        in_specs=(
            P("comp", "slab", None, None),
            P("slab", None, None),
            P("slab", None, None),
            P(None, "slab", None, None),
        ),
        out_specs=(P("comp", "slab", None, None), P("comp", "slab", None, None)),
        check_vma=False,
    )
```

```python
import functools

import jax
import jax.numpy as jnp
import numpy as np
from jax import lax
from jax.experimental import pallas as pl
from jax.experimental.pallas import tpu as pltpu
from jax.sharding import PartitionSpec as P

F32 = jnp.float32
BF16 = jnp.bfloat16
MESH = pl.DeviceIdType.MESH
ROW = 16
RING = 8
SIDE = 4
REACH = 4


def halves(table):
    table = np.asarray(table, np.float32)
    high = table.astype(BF16)
    low = (table - high.astype(np.float32)).astype(BF16)
    return high, low


def tables(n, padded):
    angle = 2.0 * np.pi / padded * (np.outer(np.arange(padded), np.arange(n)) % padded)
    cosine, sine = np.cos(angle), np.sin(angle)
    wide = np.block([[cosine, sine], [-sine, cosine]])
    planes = np.stack([part[kzb::2] for kzb in range(2) for part in (cosine, -sine)])
    return (*halves(wide), *halves(wide.T), *halves(planes))


def split(x):
    high = x.astype(BF16)
    low = (x - high.astype(F32)).astype(BF16)
    return high, low


def dot3(a, b):
    dot = functools.partial(jnp.dot, preferred_element_type=F32)
    return dot(a[0], b[0]) + dot(a[0], b[1]) + dot(a[1], b[0])


def kernel(
    n, pol_hbm, inv_hbm, occ_hbm, green_hbm, wh_hbm, wl_hbm, th_hbm, tl_hbm, ph_hbm, pl_hbm,
    out_0, out_1,
    pol, inv, occ, green, wh, wl, th, tl, ph, plo, over_x, images,
    field, inv_t, mask_t, spectrum,
    own_p, side_p, own_q, side_q,
    slab_in, part_out, part_in,
    own_s, side_s, recv, back_s, own_b, side_b,
    fwd_send, fwd_recv, back_send, back_recv, slab_send, slab_recv, part_send, part_recv, first_sem, later_sem, out_sem, met,
):
    me = lax.axis_index("slab")
    row, rank = me // ROW, lax.rem(me, ROW)
    cells = pol.shape[2]

    def at(z_row, r):
        return lax.rem(z_row + 2 * RING, RING) * ROW + r

    step_of = (1, -1)
    sides = (at(row - 1, rank), at(row + 1, rank))

    last = (REACH - 1) * ROW
    for slot in range(4):
        for side in range(2):
            side_b[slot, side, :, last:, :] = jnp.zeros((6, ROW, cells), F32)

    barrier = pltpu.get_barrier_semaphore()

    y, x = rank // SIDE, lax.rem(rank, SIDE)

    def chip(dz, dy, dx):
        to_y, to_x = lax.rem(y + dy + SIDE, SIDE), lax.rem(x + dx + SIDE, SIDE)
        return at(row + dz, to_y * SIDE + to_x)

    def greet(sem, targets):
        for shift in targets:
            pl.semaphore_signal(
                sem, inc=1, device_id={"slab": chip(*shift)}, device_id_type=MESH
            )

    def heard(sem, targets):
        pl.semaphore_wait(sem, len(targets))

    around = [(d, 0, 0) for d in (1, -1)] + [(0, d, 0) for d in (1, -1)] + [(0, 0, d) for d in (1, -1)]
    ring = [(1, 0, 0), (-1, 0, 0), (0, 0, 1), (0, 0, 2), (0, 0, 3)]
    column = [(d, 0, 0) for d in (3, -3, 2, -2, 1, -1)]
    greet(barrier, around)

    first = [
        pltpu.make_async_copy(src, dst, first_sem.at[i])
        for i, (src, dst) in enumerate(
            ((occ_hbm, occ), (pol_hbm, pol), (ph_hbm, ph), (pl_hbm, plo), (inv_hbm, inv))
        )
    ]
    later = [
        pltpu.make_async_copy(src, dst, later_sem.at[i])
        for i, (src, dst) in enumerate(
            ((wh_hbm, wh), (wl_hbm, wl), (th_hbm, th), (tl_hbm, tl), (green_hbm, green))
        )
    ]
    for copy in (*first, *later):
        copy.start()
    for copy in first:
        copy.wait()
    heard(barrier, around)
    greet(met.at[0], around)

    blocks = occ.shape[1]
    each = cells // blocks
    spread = (
        lax.broadcasted_iota(jnp.int32, (cells, blocks), 0) // each
        == lax.broadcasted_iota(jnp.int32, (cells, blocks), 1)
    ).astype(F32)
    rows = jnp.dot(spread, occ[0].astype(F32), preferred_element_type=F32)
    mask_t[...] = lax.dot_general(
        spread, rows, (((1,), (1,)), ((), ())), preferred_element_type=F32
    )
    inv_t[...] = inv[0].T
    for c in range(3):
        field[c] = pol[c, 0].T * mask_t[...]

    def slab_copy(turn, c, side):
        return pltpu.make_async_remote_copy(
            src_ref=field.at[turn * 3 + c],
            dst_ref=slab_in.at[turn, side, c],
            send_sem=slab_send.at[turn, side, c],
            recv_sem=slab_recv.at[turn, side, c],
            device_id={"slab": sides[1 - side]},
            device_id_type=MESH,
        )

    def part_copy(turn, a, side):
        return pltpu.make_async_remote_copy(
            src_ref=part_out.at[turn, side, a],
            dst_ref=part_in.at[turn, side, a],
            send_sem=part_send.at[turn, side, a],
            recv_sem=part_recv.at[turn, side, a],
            device_id={"slab": sides[side]},
            device_id_type=MESH,
        )

    def out_copy(turn, a):
        out = (out_0, out_1)[turn]
        return pltpu.make_async_copy(images.at[turn, a], out.at[a, 0], out_sem.at[turn, a])

    def send_to(src, dst, target, send_sem, recv_sem):
        pltpu.make_async_remote_copy(
            src_ref=src, dst_ref=dst, send_sem=send_sem, recv_sem=recv_sem,
            device_id={"slab": target}, device_id_type=MESH,
        ).start()

    def messages(own, side):
        @pl.loop(0, ROW // 2, unroll=2)
        def _(i):
            even = 2 * i + lax.rem(rank, 2)
            side(0, REACH - 1, even)
            side(1, REACH - 1, even ^ 1)

        for k in range(REACH - 2, 0, -1):

            @pl.loop(0, ROW, unroll=4)
            def _(r):
                side(0, k, r)
                side(1, k, r)

        @pl.loop(1, ROW, unroll=3)
        def _(i):
            r = rank ^ i
            side(0, 0, r)
            side(1, 0, r)
            own(r)

    def forward(slot, low, width, sem):
        sems = (fwd_send.at[sem], fwd_recv.at[sem])
        span = pl.ds(low, width)

        def own(r):
            send_to(
                own_s.at[slot, span, pl.ds(r, 1), :], recv.at[slot, span, pl.ds(me, 1), :],
                row * ROW + r, *sems,
            )

        def side(which, k, r):
            send_to(
                side_s.at[slot, which, span, pl.ds(k * ROW + r, 1), :],
                recv.at[slot, span, pl.ds(sides[which], 1), :],
                at(row + step_of[which] * k, r), *sems,
            )

        messages(own, side)
        recv[slot, span, pl.ds(me, 1), :] = own_s[slot, span, pl.ds(rank, 1), :]
        for which in range(2):
            recv[slot, span, pl.ds(sides[which], 1), :] = side_s[
                slot, which, span, pl.ds(rank, 1), :
            ]

    def backward(slot, low, width, sem):
        sems = (back_send.at[sem], back_recv.at[sem])
        span = pl.ds(low, width)

        def own(r):
            send_to(
                back_s.at[slot, span, pl.ds(row * ROW + r, 1), :],
                own_b.at[slot, span, pl.ds(rank, 1), :],
                row * ROW + r, *sems,
            )

        def side(which, k, r):
            collector = row - step_of[which] * k
            send_to(
                back_s.at[slot, span, pl.ds(at(collector - step_of[which], r), 1), :],
                side_b.at[slot, which, span, pl.ds(k * ROW + rank, 1), :],
                at(collector, r), *sems,
            )

        messages(own, side)
        own_b[slot, span, pl.ds(rank, 1), :] = back_s[slot, span, pl.ds(me, 1), :]
        for which in range(2):
            side_b[slot, which, span, pl.ds(rank, 1), :] = back_s[
                slot, span, pl.ds(sides[which], 1), :
            ]

    def wait_for(ref, width, sem):
        bytes_of = ref.at[0, pl.ds(0, width), pl.ds(0, n - 3), :]
        pltpu.make_async_copy(bytes_of, bytes_of, sem).wait()

    fwd_plan = ((0, 0, 2), (0, 2, 2), (0, 4, 2), (1, 0, 6))
    back_plan = ((0, 0, 6), (1, 0, 2), (1, 2, 2), (1, 4, 2))

    for c in range(3):
        for side in range(2):
            slab_copy(0, c, side).start()
    heard(met.at[0], around)
    greet(met.at[1], ring)

    for half, table in enumerate((ph, plo)):
        if half == 1:
            heard(met.at[1], ring)
            greet(met.at[2], column)
        pick = pl.ds(pl.multiple_of(row * ROW, ROW), ROW)
        own_p[half] = table[:, pick, :]
        own_q[half] = own_p[half].astype(F32).reshape(4 * ROW, cells).T.astype(BF16)
        for side in range(2):
            for k in range(REACH):
                pick = pl.ds(pl.multiple_of(at(row + step_of[side] * k, 0), ROW), ROW)
                side_p[half, side, :, k * ROW : (k + 1) * ROW, :] = table[:, pick, :]
            side_q[half, side] = (
                side_p[half, side].astype(F32).reshape(4 * REACH * ROW, cells).T.astype(BF16)
            )
    heard(met.at[2], column)

    scale = 1.0 / (8 * cells * cells * n)

    half = 2 * n
    for turn in range(2):
        slots = (2 * turn, 2 * turn + 1)
        for c in range(3):
            for side in range(2):
                slab_copy(turn, c, side).wait_recv()
            pair = slice(2 * c, 2 * c + 2)
            lhs = [own_p[part].reshape(4 * ROW, cells) for part in range(2)]
            product = dot3(lhs, split(field[turn * 3 + c])).reshape(4, ROW, cells)
            for kzb, slot in enumerate(slots):
                own_s[slot, pair] = product[2 * kzb : 2 * kzb + 2]
            for side in range(2):
                lhs = [side_p[part, side].reshape(4 * REACH * ROW, cells) for part in range(2)]
                product = dot3(lhs, split(slab_in[turn, side, c])).reshape(4, REACH * ROW, cells)
                for kzb, slot in enumerate(slots):
                    side_s[slot, side, pair] = product[2 * kzb : 2 * kzb + 2]
            forward(slots[0], 2 * c, 2, 4 * turn + c)
        forward(slots[1], 0, 6, 4 * turn + 3)

        if turn == 0:
            for copy in later:
                copy.wait()

        for kzb, slot in enumerate(slots):
            for sem, (plane, low, width) in enumerate(fwd_plan):
                if plane == kzb:
                    wait_for(recv, width, fwd_recv.at[4 * turn + sem])
            rows = split(
                jnp.concatenate(
                    [recv[slot, 2 * c : 2 * c + 2].reshape(half, cells) for c in range(3)], axis=1
                )
            )
            for part in range(2):
                at_rows = slice(part * half, (part + 1) * half)
                product = dot3((wh[at_rows], wl[at_rows]), rows)
                for c in range(3):
                    over_x[c, :, part * cells : (part + 1) * cells] = product[
                        :, c * cells : (c + 1) * cells
                    ]
            for c in range(3):
                spectrum[c] = dot3(split(over_x[c]), (th[...], tl[...]))
            for a, combo in enumerate(((0, 3, 4), (3, 1, 5), (4, 5, 2))):
                parts = [
                    green[combo[0], kzb] * spectrum[0, :, k : k + half]
                    + green[combo[1], kzb] * spectrum[1, :, k : k + half]
                    + green[combo[2], kzb] * spectrum[2, :, k : k + half]
                    for k in (0, half)
                ]
                over_y = dot3(split(jnp.concatenate(parts, axis=1)), (wh[...], wl[...]))
                both = jnp.concatenate([over_y[:, :cells], over_y[:, cells:]], axis=0)
                back_s[slot, 2 * a : 2 * a + 2] = dot3((th[...], tl[...]), split(both)).reshape(
                    2, n, cells
                )
                if kzb == 1:
                    backward(slot, 2 * a, 2, 4 * turn + 1 + a)
            if kzb == 0:
                backward(slot, 0, 6, 4 * turn)

        wait_for(recv, 6, back_recv.at[4 * turn])
        totals = []
        for a in range(3):
            wait_for(recv, 2, back_recv.at[4 * turn + 1 + a])
            for side in range(2):
                rows = jnp.concatenate(
                    [side_b[slot, side, 2 * a : 2 * a + 2].reshape(-1, cells) for slot in slots]
                )
                part_out[turn, side, a] = dot3((side_q[0, side], side_q[1, side]), split(rows))
                part_copy(turn, a, side).start()
            rows = jnp.concatenate(
                [own_b[slot, 2 * a : 2 * a + 2].reshape(-1, cells) for slot in slots]
            )
            totals.append(dot3((own_q[0], own_q[1]), split(rows)))
        for a in range(3):
            for side in range(2):
                part_copy(turn, a, side).wait_recv()
            total = totals[a] + part_in[turn, 0, a] + part_in[turn, 1, a]
            image = inv_t[...] * field[turn * 3 + a] - mask_t[...] * (total * scale)
            if turn == 0:
                field[3 + a] = image * mask_t[...]
                for side in range(2):
                    slab_copy(1, a, side).start()
            images[turn, a] = image.T
            out_copy(turn, a).start()

    for turn in range(2):
        for plan, sems in ((fwd_plan, fwd_send), (back_plan, back_send)):
            for sem, (_, _, width) in enumerate(plan):
                wait_for(recv, width, sems.at[4 * turn + sem])

    for turn in range(2):
        for c in range(3):
            out_copy(turn, c).wait()
            for side in range(2):
                slab_copy(turn, c, side).wait_send()
                part_copy(turn, c, side).wait_send()


def per_device(n, polarization, inverse_polarizability, occupancy, green_fourier):
    cells = polarization.shape[2]
    padded = green_fourier.shape[2]
    operands = (
        polarization, inverse_polarizability, occupancy, green_fourier, *tables(n, padded)
    )
    span = REACH * ROW
    image = jax.ShapeDtypeStruct(polarization.shape, F32)
    dma = pltpu.SemaphoreType.DMA
    anywhere = pl.BlockSpec(memory_space=pl.ANY)
    return pl.pallas_call(
        functools.partial(kernel, n),
        out_shape=(image, image),
        in_specs=[anywhere] * len(operands),
        out_specs=(anywhere, anywhere),
        scratch_shapes=[
            *(pltpu.VMEM(x.shape, x.dtype) for x in operands),
            pltpu.VMEM((3, padded, padded), F32),
            pltpu.VMEM((2, 3, cells, cells), F32),
            pltpu.VMEM((6, cells, cells), F32),
            pltpu.VMEM((cells, cells), F32),
            pltpu.VMEM((cells, cells), F32),
            pltpu.VMEM((3, padded, 2 * padded), F32),
            pltpu.VMEM((2, 4, ROW, cells), BF16),
            pltpu.VMEM((2, 2, 4, span, cells), BF16),
            pltpu.VMEM((2, cells, 4 * ROW), BF16),
            pltpu.VMEM((2, 2, cells, 4 * span), BF16),
            pltpu.VMEM((2, 2, 3, cells, cells), F32),
            pltpu.VMEM((2, 2, 3, cells, cells), F32),
            pltpu.VMEM((2, 2, 3, cells, cells), F32),
            pltpu.VMEM((4, 6, ROW, cells), F32),
            pltpu.VMEM((4, 2, 6, span, cells), F32),
            pltpu.VMEM((4, 6, n, cells), F32),
            pltpu.VMEM((4, 6, n, cells), F32),
            pltpu.VMEM((4, 6, ROW, cells), F32),
            pltpu.VMEM((4, 2, 6, span, cells), F32),
            dma((8,)), dma((8,)), dma((8,)), dma((8,)),
            dma((2, 2, 3)), dma((2, 2, 3)), dma((2, 2, 3)), dma((2, 2, 3)), dma((5,)), dma((5,)), dma((2, 3)),
            pltpu.SemaphoreType.REGULAR((3,)),
        ],
        compiler_params=pltpu.CompilerParams(
            has_side_effects=True, collective_id=0, vmem_limit_bytes=56 * 2**20
        ),
    )(*operands)


def solution(mesh):
    return jax.shard_map(
        functools.partial(per_device, mesh.shape["slab"]),
        mesh=mesh,
        in_specs=(
            P("comp", "slab", None, None),
            P("slab", None, None),
            P("slab", None, None),
            P(None, "slab", None, None),
        ),
        out_specs=(P("comp", "slab", None, None), P("comp", "slab", None, None)),
        check_vma=False,
    )
```

```python
import functools

import jax
import jax.numpy as jnp
import numpy as np
from jax import lax
from jax.experimental import pallas as pl
from jax.experimental.pallas import tpu as pltpu
from jax.sharding import PartitionSpec as P

F32 = jnp.float32
BF16 = jnp.bfloat16
MESH = pl.DeviceIdType.MESH
ROW = 16
RING = 8
SIDE = 4
REACH = 4


def halves(table):
    table = np.asarray(table, np.float32)
    high = table.astype(BF16)
    low = (table - high.astype(np.float32)).astype(BF16)
    return high, low


def tables(n, padded):
    angle = 2.0 * np.pi / padded * (np.outer(np.arange(padded), np.arange(n)) % padded)
    cosine, sine = np.cos(angle), np.sin(angle)
    wide = np.block([[cosine, sine], [-sine, cosine]])
    planes = np.stack([part[kzb::2] for kzb in range(2) for part in (cosine, -sine)])
    return (*halves(wide), *halves(wide.T), *halves(planes))


def split(x):
    high = x.astype(BF16)
    low = (x - high.astype(F32)).astype(BF16)
    return high, low


def dot3(a, b):
    dot = functools.partial(jnp.dot, preferred_element_type=F32)
    return dot(a[0], b[0]) + dot(a[0], b[1]) + dot(a[1], b[0])


def kernel(
    n, pol_hbm, inv_hbm, occ_hbm, green_hbm, wh_hbm, wl_hbm, th_hbm, tl_hbm, ph_hbm, pl_hbm,
    out_0, out_1,
    pol, inv, occ, green, wh, wl, th, tl, ph, plo, over_x, images,
    field, inv_t, mask_t, spectrum,
    own_p, side_p, own_q, side_q,
    slab_in, part_out, part_in,
    own_s, side_s, recv, back_s, own_b, side_b,
    fwd_send, fwd_recv, back_send, back_recv, slab_send, slab_recv, part_send, part_recv, first_sem, later_sem, out_sem, met,
):
    me = lax.axis_index("slab")
    row, rank = me // ROW, lax.rem(me, ROW)
    cells = pol.shape[2]

    def at(z_row, r):
        return lax.rem(z_row + 2 * RING, RING) * ROW + r

    step_of = (1, -1)
    sides = (at(row - 1, rank), at(row + 1, rank))

    last = (REACH - 1) * ROW
    for slot in range(4):
        for side in range(2):
            side_b[slot, side, :, last:, :] = jnp.zeros((6, ROW, cells), F32)

    barrier = pltpu.get_barrier_semaphore()

    y, x = rank // SIDE, lax.rem(rank, SIDE)

    def chip(dz, dy, dx):
        to_y, to_x = lax.rem(y + dy + SIDE, SIDE), lax.rem(x + dx + SIDE, SIDE)
        return at(row + dz, to_y * SIDE + to_x)

    def greet(sem, targets):
        for shift in targets:
            pl.semaphore_signal(
                sem, inc=1, device_id={"slab": chip(*shift)}, device_id_type=MESH
            )

    def heard(sem, targets):
        pl.semaphore_wait(sem, len(targets))

    around = [(d, 0, 0) for d in (1, -1)] + [(0, d, 0) for d in (1, -1)] + [(0, 0, d) for d in (1, -1)]
    ring = [(1, 0, 0), (-1, 0, 0), (0, 0, 1), (0, 0, 2), (0, 0, 3)]
    column = [(d, 0, 0) for d in (3, -3, 2, -2, 1, -1)]
    greet(barrier, around)

    first = [
        pltpu.make_async_copy(src, dst, first_sem.at[i])
        for i, (src, dst) in enumerate(
            ((occ_hbm, occ), (pol_hbm, pol), (ph_hbm, ph), (pl_hbm, plo), (inv_hbm, inv))
        )
    ]
    later = [
        pltpu.make_async_copy(src, dst, later_sem.at[i])
        for i, (src, dst) in enumerate(
            ((wh_hbm, wh), (wl_hbm, wl), (th_hbm, th), (tl_hbm, tl), (green_hbm, green))
        )
    ]
    for copy in (*first, *later):
        copy.start()
    for copy in first:
        copy.wait()
    heard(barrier, around)
    greet(met.at[0], around)

    blocks = occ.shape[1]
    each = cells // blocks
    spread = (
        lax.broadcasted_iota(jnp.int32, (cells, blocks), 0) // each
        == lax.broadcasted_iota(jnp.int32, (cells, blocks), 1)
    ).astype(F32)
    rows = jnp.dot(spread, occ[0].astype(F32), preferred_element_type=F32)
    mask_t[...] = lax.dot_general(
        spread, rows, (((1,), (1,)), ((), ())), preferred_element_type=F32
    )
    inv_t[...] = inv[0].T
    for c in range(3):
        field[c] = pol[c, 0].T * mask_t[...]

    def slab_copy(turn, c, side):
        return pltpu.make_async_remote_copy(
            src_ref=field.at[turn * 3 + c],
            dst_ref=slab_in.at[turn, side, c],
            send_sem=slab_send.at[turn, side, c],
            recv_sem=slab_recv.at[turn, side, c],
            device_id={"slab": sides[1 - side]},
            device_id_type=MESH,
        )

    def part_copy(turn, a, side):
        return pltpu.make_async_remote_copy(
            src_ref=part_out.at[turn, side, a],
            dst_ref=part_in.at[turn, side, a],
            send_sem=part_send.at[turn, side, a],
            recv_sem=part_recv.at[turn, side, a],
            device_id={"slab": sides[side]},
            device_id_type=MESH,
        )

    def out_copy(turn, a):
        out = (out_0, out_1)[turn]
        return pltpu.make_async_copy(images.at[turn, a], out.at[a, 0], out_sem.at[turn, a])

    def send_to(src, dst, target, send_sem, recv_sem):
        pltpu.make_async_remote_copy(
            src_ref=src, dst_ref=dst, send_sem=send_sem, recv_sem=recv_sem,
            device_id={"slab": target}, device_id_type=MESH,
        ).start()

    def messages(own, side):
        @pl.loop(0, ROW // 2, unroll=2)
        def _(i):
            even = 2 * i + lax.rem(rank, 2)
            side(0, REACH - 1, even)
            side(1, REACH - 1, even ^ 1)

        for k in range(REACH - 2, 0, -1):

            @pl.loop(0, ROW, unroll=4)
            def _(r):
                side(0, k, r)
                side(1, k, r)

        @pl.loop(1, ROW, unroll=3)
        def _(i):
            r = rank ^ i
            side(0, 0, r)
            side(1, 0, r)
            own(r)

    def forward(slot, low, width, sem):
        sems = (fwd_send.at[sem], fwd_recv.at[sem])
        span = pl.ds(low, width)

        def own(r):
            send_to(
                own_s.at[slot, span, pl.ds(r, 1), :], recv.at[slot, span, pl.ds(me, 1), :],
                row * ROW + r, *sems,
            )

        def side(which, k, r):
            send_to(
                side_s.at[slot, which, span, pl.ds(k * ROW + r, 1), :],
                recv.at[slot, span, pl.ds(sides[which], 1), :],
                at(row + step_of[which] * k, r), *sems,
            )

        messages(own, side)
        recv[slot, span, pl.ds(me, 1), :] = own_s[slot, span, pl.ds(rank, 1), :]
        for which in range(2):
            recv[slot, span, pl.ds(sides[which], 1), :] = side_s[
                slot, which, span, pl.ds(rank, 1), :
            ]

    def backward(slot, low, width, sem):
        sems = (back_send.at[sem], back_recv.at[sem])
        span = pl.ds(low, width)

        def own(r):
            send_to(
                back_s.at[slot, span, pl.ds(row * ROW + r, 1), :],
                own_b.at[slot, span, pl.ds(rank, 1), :],
                row * ROW + r, *sems,
            )

        def side(which, k, r):
            collector = row - step_of[which] * k
            send_to(
                back_s.at[slot, span, pl.ds(at(collector - step_of[which], r), 1), :],
                side_b.at[slot, which, span, pl.ds(k * ROW + rank, 1), :],
                at(collector, r), *sems,
            )

        messages(own, side)
        own_b[slot, span, pl.ds(rank, 1), :] = back_s[slot, span, pl.ds(me, 1), :]
        for which in range(2):
            side_b[slot, which, span, pl.ds(rank, 1), :] = back_s[
                slot, span, pl.ds(sides[which], 1), :
            ]

    def wait_for(ref, width, sem):
        bytes_of = ref.at[0, pl.ds(0, width), pl.ds(0, n - 3), :]
        pltpu.make_async_copy(bytes_of, bytes_of, sem).wait()

    fwd_plan = ((0, 0, 2), (0, 2, 2), (0, 4, 2), (1, 0, 6))
    back_plan = ((0, 0, 6), (1, 0, 2), (1, 2, 2), (1, 4, 2))

    for c in range(3):
        for side in range(2):
            slab_copy(0, c, side).start()
    heard(met.at[0], around)
    greet(met.at[1], ring)

    for half, table in enumerate((ph, plo)):
        if half == 1:
            heard(met.at[1], ring)
            greet(met.at[2], column)
        pick = pl.ds(pl.multiple_of(row * ROW, ROW), ROW)
        own_p[half] = table[:, pick, :]
        own_q[half] = own_p[half].astype(F32).reshape(4 * ROW, cells).T.astype(BF16)
        for side in range(2):
            for k in range(REACH):
                pick = pl.ds(pl.multiple_of(at(row + step_of[side] * k, 0), ROW), ROW)
                side_p[half, side, :, k * ROW : (k + 1) * ROW, :] = table[:, pick, :]
            side_q[half, side] = (
                side_p[half, side].astype(F32).reshape(4 * REACH * ROW, cells).T.astype(BF16)
            )
    heard(met.at[2], column)

    scale = 1.0 / (8 * cells * cells * n)

    half = 2 * n
    for turn in range(2):
        slots = (2 * turn, 2 * turn + 1)
        for c in range(3):
            for side in range(2):
                slab_copy(turn, c, side).wait_recv()
            pair = slice(2 * c, 2 * c + 2)
            lhs = [own_p[part].reshape(4 * ROW, cells) for part in range(2)]
            product = dot3(lhs, split(field[turn * 3 + c])).reshape(4, ROW, cells)
            for kzb, slot in enumerate(slots):
                own_s[slot, pair] = product[2 * kzb : 2 * kzb + 2]
            for side in range(2):
                lhs = [side_p[part, side].reshape(4 * REACH * ROW, cells) for part in range(2)]
                product = dot3(lhs, split(slab_in[turn, side, c])).reshape(4, REACH * ROW, cells)
                for kzb, slot in enumerate(slots):
                    side_s[slot, side, pair] = product[2 * kzb : 2 * kzb + 2]
            forward(slots[0], 2 * c, 2, 4 * turn + c)
        forward(slots[1], 0, 6, 4 * turn + 3)

        if turn == 0:
            for copy in later:
                copy.wait()

        for kzb, slot in enumerate(slots):
            for sem, (plane, low, width) in enumerate(fwd_plan):
                if plane != kzb:
                    continue
                wait_for(recv, width, fwd_recv.at[4 * turn + sem])
                components = range(low // 2, (low + width) // 2)
                rows = split(
                    jnp.concatenate(
                        [recv[slot, 2 * c : 2 * c + 2].reshape(half, cells) for c in components],
                        axis=1,
                    )
                )
                for part in range(2):
                    at_rows = slice(part * half, (part + 1) * half)
                    product = dot3((wh[at_rows], wl[at_rows]), rows)
                    for i, c in enumerate(components):
                        over_x[c, :, part * cells : (part + 1) * cells] = product[
                            :, i * cells : (i + 1) * cells
                        ]
                for c in components:
                    spectrum[c] = dot3(split(over_x[c]), (th[...], tl[...]))
            for a, combo in enumerate(((0, 3, 4), (3, 1, 5), (4, 5, 2))):
                parts = [
                    green[combo[0], kzb] * spectrum[0, :, k : k + half]
                    + green[combo[1], kzb] * spectrum[1, :, k : k + half]
                    + green[combo[2], kzb] * spectrum[2, :, k : k + half]
                    for k in (0, half)
                ]
                over_y = dot3(split(jnp.concatenate(parts, axis=1)), (wh[...], wl[...]))
                both = jnp.concatenate([over_y[:, :cells], over_y[:, cells:]], axis=0)
                back_s[slot, 2 * a : 2 * a + 2] = dot3((th[...], tl[...]), split(both)).reshape(
                    2, n, cells
                )
                if kzb == 1:
                    backward(slot, 2 * a, 2, 4 * turn + 1 + a)
            if kzb == 0:
                backward(slot, 0, 6, 4 * turn)

        wait_for(recv, 6, back_recv.at[4 * turn])
        totals = []
        for a in range(3):
            wait_for(recv, 2, back_recv.at[4 * turn + 1 + a])
            for side in range(2):
                rows = jnp.concatenate(
                    [side_b[slot, side, 2 * a : 2 * a + 2].reshape(-1, cells) for slot in slots]
                )
                part_out[turn, side, a] = dot3((side_q[0, side], side_q[1, side]), split(rows))
                part_copy(turn, a, side).start()
            rows = jnp.concatenate(
                [own_b[slot, 2 * a : 2 * a + 2].reshape(-1, cells) for slot in slots]
            )
            totals.append(dot3((own_q[0], own_q[1]), split(rows)))
        for a in range(3):
            for side in range(2):
                part_copy(turn, a, side).wait_recv()
            total = totals[a] + part_in[turn, 0, a] + part_in[turn, 1, a]
            image = inv_t[...] * field[turn * 3 + a] - mask_t[...] * (total * scale)
            if turn == 0:
                field[3 + a] = image * mask_t[...]
                for side in range(2):
                    slab_copy(1, a, side).start()
            images[turn, a] = image.T
            out_copy(turn, a).start()

    for turn in range(2):
        for plan, sems in ((fwd_plan, fwd_send), (back_plan, back_send)):
            for sem, (_, _, width) in enumerate(plan):
                wait_for(recv, width, sems.at[4 * turn + sem])

    for turn in range(2):
        for c in range(3):
            out_copy(turn, c).wait()
            for side in range(2):
                slab_copy(turn, c, side).wait_send()
                part_copy(turn, c, side).wait_send()


def per_device(n, polarization, inverse_polarizability, occupancy, green_fourier):
    cells = polarization.shape[2]
    padded = green_fourier.shape[2]
    operands = (
        polarization, inverse_polarizability, occupancy, green_fourier, *tables(n, padded)
    )
    span = REACH * ROW
    image = jax.ShapeDtypeStruct(polarization.shape, F32)
    dma = pltpu.SemaphoreType.DMA
    anywhere = pl.BlockSpec(memory_space=pl.ANY)
    return pl.pallas_call(
        functools.partial(kernel, n),
        out_shape=(image, image),
        in_specs=[anywhere] * len(operands),
        out_specs=(anywhere, anywhere),
        scratch_shapes=[
            *(pltpu.VMEM(x.shape, x.dtype) for x in operands),
            pltpu.VMEM((3, padded, padded), F32),
            pltpu.VMEM((2, 3, cells, cells), F32),
            pltpu.VMEM((6, cells, cells), F32),
            pltpu.VMEM((cells, cells), F32),
            pltpu.VMEM((cells, cells), F32),
            pltpu.VMEM((3, padded, 2 * padded), F32),
            pltpu.VMEM((2, 4, ROW, cells), BF16),
            pltpu.VMEM((2, 2, 4, span, cells), BF16),
            pltpu.VMEM((2, cells, 4 * ROW), BF16),
            pltpu.VMEM((2, 2, cells, 4 * span), BF16),
            pltpu.VMEM((2, 2, 3, cells, cells), F32),
            pltpu.VMEM((2, 2, 3, cells, cells), F32),
            pltpu.VMEM((2, 2, 3, cells, cells), F32),
            pltpu.VMEM((4, 6, ROW, cells), F32),
            pltpu.VMEM((4, 2, 6, span, cells), F32),
            pltpu.VMEM((4, 6, n, cells), F32),
            pltpu.VMEM((4, 6, n, cells), F32),
            pltpu.VMEM((4, 6, ROW, cells), F32),
            pltpu.VMEM((4, 2, 6, span, cells), F32),
            dma((8,)), dma((8,)), dma((8,)), dma((8,)),
            dma((2, 2, 3)), dma((2, 2, 3)), dma((2, 2, 3)), dma((2, 2, 3)), dma((5,)), dma((5,)), dma((2, 3)),
            pltpu.SemaphoreType.REGULAR((3,)),
        ],
        compiler_params=pltpu.CompilerParams(
            has_side_effects=True, collective_id=0, vmem_limit_bytes=56 * 2**20
        ),
    )(*operands)


def solution(mesh):
    return jax.shard_map(
        functools.partial(per_device, mesh.shape["slab"]),
        mesh=mesh,
        in_specs=(
            P("comp", "slab", None, None),
            P("slab", None, None),
            P("slab", None, None),
            P(None, "slab", None, None),
        ),
        out_specs=(P("comp", "slab", None, None), P("comp", "slab", None, None)),
        check_vma=False,
    )
```

```python
import functools

import jax
import jax.numpy as jnp
import numpy as np
from jax import lax
from jax.experimental import pallas as pl
from jax.experimental.pallas import tpu as pltpu
from jax.sharding import PartitionSpec as P

F32 = jnp.float32
BF16 = jnp.bfloat16
MESH = pl.DeviceIdType.MESH
ROW = 16
RING = 8
SIDE = 4
REACH = 4


def halves(table):
    table = np.asarray(table, np.float32)
    high = table.astype(BF16)
    low = (table - high.astype(np.float32)).astype(BF16)
    return high, low


def tables(n, padded):
    angle = 2.0 * np.pi / padded * (np.outer(np.arange(padded), np.arange(n)) % padded)
    cosine, sine = np.cos(angle), np.sin(angle)
    wide = np.block([[cosine, sine], [-sine, cosine]])
    planes = np.stack([part[kzb::2] for kzb in range(2) for part in (cosine, -sine)])
    return (*halves(wide), *halves(wide.T), *halves(planes))


def split(x):
    high = x.astype(BF16)
    low = (x - high.astype(F32)).astype(BF16)
    return high, low


def dot3(a, b):
    dot = functools.partial(jnp.dot, preferred_element_type=F32)
    return dot(a[0], b[0]) + dot(a[0], b[1]) + dot(a[1], b[0])


def kernel(
    n, pol_hbm, inv_hbm, occ_hbm, green_hbm, wh_hbm, wl_hbm, th_hbm, tl_hbm, ph_hbm, pl_hbm,
    out_0, out_1,
    pol, inv, occ, green, wh, wl, th, tl, ph, plo, over_x, images,
    field, inv_t, mask_t, spectrum,
    own_p, side_p, own_q, side_q,
    slab_in, part_out, part_in,
    own_s, side_s, recv, back_s, own_b, side_b,
    fwd_send, fwd_recv, back_send, back_recv, slab_send, slab_recv, part_send, part_recv, first_sem, later_sem, out_sem, met,
):
    me = lax.axis_index("slab")
    row, rank = me // ROW, lax.rem(me, ROW)
    cells = pol.shape[2]

    def at(z_row, r):
        return lax.rem(z_row + 2 * RING, RING) * ROW + r

    step_of = (1, -1)
    sides = (at(row - 1, rank), at(row + 1, rank))

    last = (REACH - 1) * ROW
    for slot in range(4):
        for side in range(2):
            side_b[slot, side, :, last:, :] = jnp.zeros((6, ROW, cells), F32)

    barrier = pltpu.get_barrier_semaphore()

    y, x = rank // SIDE, lax.rem(rank, SIDE)

    def chip(dz, dy, dx):
        to_y, to_x = lax.rem(y + dy + SIDE, SIDE), lax.rem(x + dx + SIDE, SIDE)
        return at(row + dz, to_y * SIDE + to_x)

    def greet(sem, targets):
        for shift in targets:
            pl.semaphore_signal(
                sem, inc=1, device_id={"slab": chip(*shift)}, device_id_type=MESH
            )

    def heard(sem, targets):
        pl.semaphore_wait(sem, len(targets))

    around = [(d, 0, 0) for d in (1, -1)] + [(0, d, 0) for d in (1, -1)] + [(0, 0, d) for d in (1, -1)]
    ring = [(1, 0, 0), (-1, 0, 0), (0, 0, 1), (0, 0, 2), (0, 0, 3)]
    column = [(d, 0, 0) for d in (3, -3, 2, -2, 1, -1)]
    greet(barrier, around)

    first = [
        pltpu.make_async_copy(src, dst, first_sem.at[i])
        for i, (src, dst) in enumerate(
            ((occ_hbm, occ), (pol_hbm, pol), (ph_hbm, ph), (pl_hbm, plo), (inv_hbm, inv))
        )
    ]
    later = [
        pltpu.make_async_copy(src, dst, later_sem.at[i])
        for i, (src, dst) in enumerate(
            ((wh_hbm, wh), (wl_hbm, wl), (th_hbm, th), (tl_hbm, tl), (green_hbm, green))
        )
    ]
    for copy in (*first, *later):
        copy.start()
    for copy in first[:2]:
        copy.wait()
    heard(barrier, around)
    greet(met.at[0], around)

    blocks = occ.shape[1]
    each = cells // blocks
    spread = (
        lax.broadcasted_iota(jnp.int32, (cells, blocks), 0) // each
        == lax.broadcasted_iota(jnp.int32, (cells, blocks), 1)
    ).astype(F32)
    rows = jnp.dot(spread, occ[0].astype(F32), preferred_element_type=F32)
    mask_t[...] = lax.dot_general(
        spread, rows, (((1,), (1,)), ((), ())), preferred_element_type=F32
    )
    for c in range(3):
        field[c] = pol[c, 0].T * mask_t[...]

    def slab_copy(turn, c, side):
        return pltpu.make_async_remote_copy(
            src_ref=field.at[turn * 3 + c],
            dst_ref=slab_in.at[turn, side, c],
            send_sem=slab_send.at[turn, side, c],
            recv_sem=slab_recv.at[turn, side, c],
            device_id={"slab": sides[1 - side]},
            device_id_type=MESH,
        )

    def part_copy(turn, a, side):
        return pltpu.make_async_remote_copy(
            src_ref=part_out.at[turn, side, a],
            dst_ref=part_in.at[turn, side, a],
            send_sem=part_send.at[turn, side, a],
            recv_sem=part_recv.at[turn, side, a],
            device_id={"slab": sides[side]},
            device_id_type=MESH,
        )

    def out_copy(turn, a):
        out = (out_0, out_1)[turn]
        return pltpu.make_async_copy(images.at[turn, a], out.at[a, 0], out_sem.at[turn, a])

    def send_to(src, dst, target, send_sem, recv_sem):
        pltpu.make_async_remote_copy(
            src_ref=src, dst_ref=dst, send_sem=send_sem, recv_sem=recv_sem,
            device_id={"slab": target}, device_id_type=MESH,
        ).start()

    def messages(own, side):
        @pl.loop(0, ROW // 2, unroll=2)
        def _(i):
            even = 2 * i + lax.rem(rank, 2)
            side(0, REACH - 1, even)
            side(1, REACH - 1, even ^ 1)

        for k in range(REACH - 2, 0, -1):

            @pl.loop(0, ROW, unroll=4)
            def _(r):
                side(0, k, r)
                side(1, k, r)

        @pl.loop(1, ROW, unroll=3)
        def _(i):
            r = rank ^ i
            side(0, 0, r)
            side(1, 0, r)
            own(r)

    def forward(slot, low, width, sem):
        sems = (fwd_send.at[sem], fwd_recv.at[sem])
        span = pl.ds(low, width)

        def own(r):
            send_to(
                own_s.at[slot, span, pl.ds(r, 1), :], recv.at[slot, span, pl.ds(me, 1), :],
                row * ROW + r, *sems,
            )

        def side(which, k, r):
            send_to(
                side_s.at[slot, which, span, pl.ds(k * ROW + r, 1), :],
                recv.at[slot, span, pl.ds(sides[which], 1), :],
                at(row + step_of[which] * k, r), *sems,
            )

        messages(own, side)
        recv[slot, span, pl.ds(me, 1), :] = own_s[slot, span, pl.ds(rank, 1), :]
        for which in range(2):
            recv[slot, span, pl.ds(sides[which], 1), :] = side_s[
                slot, which, span, pl.ds(rank, 1), :
            ]

    def backward(slot, low, width, sem):
        sems = (back_send.at[sem], back_recv.at[sem])
        span = pl.ds(low, width)

        def own(r):
            send_to(
                back_s.at[slot, span, pl.ds(row * ROW + r, 1), :],
                own_b.at[slot, span, pl.ds(rank, 1), :],
                row * ROW + r, *sems,
            )

        def side(which, k, r):
            collector = row - step_of[which] * k
            send_to(
                back_s.at[slot, span, pl.ds(at(collector - step_of[which], r), 1), :],
                side_b.at[slot, which, span, pl.ds(k * ROW + rank, 1), :],
                at(collector, r), *sems,
            )

        messages(own, side)
        own_b[slot, span, pl.ds(rank, 1), :] = back_s[slot, span, pl.ds(me, 1), :]
        for which in range(2):
            side_b[slot, which, span, pl.ds(rank, 1), :] = back_s[
                slot, span, pl.ds(sides[which], 1), :
            ]

    def wait_for(ref, width, sem):
        bytes_of = ref.at[0, pl.ds(0, width), pl.ds(0, n - 3), :]
        pltpu.make_async_copy(bytes_of, bytes_of, sem).wait()

    fwd_plan = ((0, 0, 2), (0, 2, 2), (0, 4, 2), (1, 0, 6))
    back_plan = ((0, 0, 6), (1, 0, 2), (1, 2, 2), (1, 4, 2))

    for c in range(3):
        for side in range(2):
            slab_copy(0, c, side).start()
    heard(met.at[0], around)
    greet(met.at[1], ring)
    for copy in first[2:]:
        copy.wait()
    inv_t[...] = inv[0].T

    for half, table in enumerate((ph, plo)):
        if half == 1:
            heard(met.at[1], ring)
            greet(met.at[2], column)
        pick = pl.ds(pl.multiple_of(row * ROW, ROW), ROW)
        own_p[half] = table[:, pick, :]
        own_q[half] = own_p[half].astype(F32).reshape(4 * ROW, cells).T.astype(BF16)
        for side in range(2):
            for k in range(REACH):
                pick = pl.ds(pl.multiple_of(at(row + step_of[side] * k, 0), ROW), ROW)
                side_p[half, side, :, k * ROW : (k + 1) * ROW, :] = table[:, pick, :]
            side_q[half, side] = (
                side_p[half, side].astype(F32).reshape(4 * REACH * ROW, cells).T.astype(BF16)
            )
    heard(met.at[2], column)

    scale = 1.0 / (8 * cells * cells * n)

    half = 2 * n
    for turn in range(2):
        slots = (2 * turn, 2 * turn + 1)
        for c in range(3):
            for side in range(2):
                slab_copy(turn, c, side).wait_recv()
            pair = slice(2 * c, 2 * c + 2)
            lhs = [own_p[part].reshape(4 * ROW, cells) for part in range(2)]
            product = dot3(lhs, split(field[turn * 3 + c])).reshape(4, ROW, cells)
            for kzb, slot in enumerate(slots):
                own_s[slot, pair] = product[2 * kzb : 2 * kzb + 2]
            for side in range(2):
                lhs = [side_p[part, side].reshape(4 * REACH * ROW, cells) for part in range(2)]
                product = dot3(lhs, split(slab_in[turn, side, c])).reshape(4, REACH * ROW, cells)
                for kzb, slot in enumerate(slots):
                    side_s[slot, side, pair] = product[2 * kzb : 2 * kzb + 2]
            forward(slots[0], 2 * c, 2, 4 * turn + c)
        forward(slots[1], 0, 6, 4 * turn + 3)

        if turn == 0:
            for copy in later:
                copy.wait()

        for kzb, slot in enumerate(slots):
            for sem, (plane, low, width) in enumerate(fwd_plan):
                if plane != kzb:
                    continue
                wait_for(recv, width, fwd_recv.at[4 * turn + sem])
                components = range(low // 2, (low + width) // 2)
                rows = split(
                    jnp.concatenate(
                        [recv[slot, 2 * c : 2 * c + 2].reshape(half, cells) for c in components],
                        axis=1,
                    )
                )
                for part in range(2):
                    at_rows = slice(part * half, (part + 1) * half)
                    product = dot3((wh[at_rows], wl[at_rows]), rows)
                    for i, c in enumerate(components):
                        over_x[c, :, part * cells : (part + 1) * cells] = product[
                            :, i * cells : (i + 1) * cells
                        ]
                for c in components:
                    spectrum[c] = dot3(split(over_x[c]), (th[...], tl[...]))
            stacked = []
            for a, combo in enumerate(((0, 3, 4), (3, 1, 5), (4, 5, 2))):
                parts = [
                    green[combo[0], kzb] * spectrum[0, :, k : k + half]
                    + green[combo[1], kzb] * spectrum[1, :, k : k + half]
                    + green[combo[2], kzb] * spectrum[2, :, k : k + half]
                    for k in (0, half)
                ]
                over_y = dot3(split(jnp.concatenate(parts, axis=1)), (wh[...], wl[...]))
                both = jnp.concatenate([over_y[:, :cells], over_y[:, cells:]], axis=0)
                if kzb == 0:
                    stacked.append(both)
                    continue
                back_s[slot, 2 * a : 2 * a + 2] = dot3((th[...], tl[...]), split(both)).reshape(
                    2, n, cells
                )
                backward(slot, 2 * a, 2, 4 * turn + 1 + a)
            if kzb == 0:
                product = dot3((th[...], tl[...]), split(jnp.concatenate(stacked, axis=1)))
                for a in range(3):
                    back_s[slot, 2 * a : 2 * a + 2] = product[
                        :, a * cells : (a + 1) * cells
                    ].reshape(2, n, cells)
                backward(slot, 0, 6, 4 * turn)

        wait_for(recv, 6, back_recv.at[4 * turn])
        totals = []
        for a in range(3):
            wait_for(recv, 2, back_recv.at[4 * turn + 1 + a])
            for side in range(2):
                rows = jnp.concatenate(
                    [side_b[slot, side, 2 * a : 2 * a + 2].reshape(-1, cells) for slot in slots]
                )
                part_out[turn, side, a] = dot3((side_q[0, side], side_q[1, side]), split(rows))
                part_copy(turn, a, side).start()
            rows = jnp.concatenate(
                [own_b[slot, 2 * a : 2 * a + 2].reshape(-1, cells) for slot in slots]
            )
            totals.append(dot3((own_q[0], own_q[1]), split(rows)))
        for a in range(3):
            for side in range(2):
                part_copy(turn, a, side).wait_recv()
            total = totals[a] + part_in[turn, 0, a] + part_in[turn, 1, a]
            image = inv_t[...] * field[turn * 3 + a] - mask_t[...] * (total * scale)
            if turn == 0:
                field[3 + a] = image * mask_t[...]
                for side in range(2):
                    slab_copy(1, a, side).start()
            images[turn, a] = image.T
            out_copy(turn, a).start()

    for turn in range(2):
        for plan, sems in ((fwd_plan, fwd_send), (back_plan, back_send)):
            for sem, (_, _, width) in enumerate(plan):
                wait_for(recv, width, sems.at[4 * turn + sem])

    for turn in range(2):
        for c in range(3):
            out_copy(turn, c).wait()
            for side in range(2):
                slab_copy(turn, c, side).wait_send()
                part_copy(turn, c, side).wait_send()


def per_device(n, polarization, inverse_polarizability, occupancy, green_fourier):
    cells = polarization.shape[2]
    padded = green_fourier.shape[2]
    operands = (
        polarization, inverse_polarizability, occupancy, green_fourier, *tables(n, padded)
    )
    span = REACH * ROW
    image = jax.ShapeDtypeStruct(polarization.shape, F32)
    dma = pltpu.SemaphoreType.DMA
    anywhere = pl.BlockSpec(memory_space=pl.ANY)
    return pl.pallas_call(
        functools.partial(kernel, n),
        out_shape=(image, image),
        in_specs=[anywhere] * len(operands),
        out_specs=(anywhere, anywhere),
        scratch_shapes=[
            *(pltpu.VMEM(x.shape, x.dtype) for x in operands),
            pltpu.VMEM((3, padded, padded), F32),
            pltpu.VMEM((2, 3, cells, cells), F32),
            pltpu.VMEM((6, cells, cells), F32),
            pltpu.VMEM((cells, cells), F32),
            pltpu.VMEM((cells, cells), F32),
            pltpu.VMEM((3, padded, 2 * padded), F32),
            pltpu.VMEM((2, 4, ROW, cells), BF16),
            pltpu.VMEM((2, 2, 4, span, cells), BF16),
            pltpu.VMEM((2, cells, 4 * ROW), BF16),
            pltpu.VMEM((2, 2, cells, 4 * span), BF16),
            pltpu.VMEM((2, 2, 3, cells, cells), F32),
            pltpu.VMEM((2, 2, 3, cells, cells), F32),
            pltpu.VMEM((2, 2, 3, cells, cells), F32),
            pltpu.VMEM((4, 6, ROW, cells), F32),
            pltpu.VMEM((4, 2, 6, span, cells), F32),
            pltpu.VMEM((4, 6, n, cells), F32),
            pltpu.VMEM((4, 6, n, cells), F32),
            pltpu.VMEM((4, 6, ROW, cells), F32),
            pltpu.VMEM((4, 2, 6, span, cells), F32),
            dma((8,)), dma((8,)), dma((8,)), dma((8,)),
            dma((2, 2, 3)), dma((2, 2, 3)), dma((2, 2, 3)), dma((2, 2, 3)), dma((5,)), dma((5,)), dma((2, 3)),
            pltpu.SemaphoreType.REGULAR((3,)),
        ],
        compiler_params=pltpu.CompilerParams(
            has_side_effects=True, collective_id=0, vmem_limit_bytes=56 * 2**20
        ),
    )(*operands)


def solution(mesh):
    return jax.shard_map(
        functools.partial(per_device, mesh.shape["slab"]),
        mesh=mesh,
        in_specs=(
            P("comp", "slab", None, None),
            P("slab", None, None),
            P("slab", None, None),
            P(None, "slab", None, None),
        ),
        out_specs=(P("comp", "slab", None, None), P("comp", "slab", None, None)),
        check_vma=False,
    )
```
